32 devices in a mesh: head: 4 (over z), seq: 8 (over y, x, core).
Axes of the slice: x: 2, y: 2, z: 4, core: 2. Of those that a mesh axis runs over, the one named last changes fastest.
Arguments:
- queries: bfloat16 [1024, 8192], P('seq', 'head'), may hold values from -100 to 100
- keys: bfloat16 [1024, 1024], P('seq', 'head'), may hold values from -5 to 5
- values: bfloat16 [1024, 1024], P('seq', 'head'), may hold values from -6 to 6
- q_tangent: bfloat16 [1024, 8192], P('seq', 'head'), may hold values from -6 to 6
- k_tangent: bfloat16 [1024, 1024], P('seq', 'head'), may hold values from -6 to 6
- v_tangent: bfloat16 [1024, 1024], P('seq', 'head'), may hold values from -6 to 6
- out_grad: bfloat16 [1024, 8192], P('seq', 'head'), may hold values from -6 to 6
- block_order: int32 [8], replicated, may hold values from 0 to 7, each once
Outputs:
- dq_tangent: bfloat16 [1024, 8192], P('seq', 'head')
- dk_tangent: bfloat16 [1024, 1024], P('seq', 'head')
- dv_tangent: bfloat16 [1024, 1024], P('seq', 'head')
- squared_norm: float32 [], replicated
The draws below stay inside these ranges and needn't reach their ends.
Inputs may be any that keep to these rules, and one draw needn't show every extreme that they name: `block_order`: every value of 0 to 7 appears once.
All inputs are finite; a program needn't handle non-finite values.
Results may differ from the reference program's by a relative error of at most 0.025.
Values may be sent and summed in bfloat16 or wider, within the bound.
No kernel may reach another device: no remote copies, remote signals or barrier semaphores. Data moves between devices by JAX's collectives and lax.ppermute only.
A program may use at most 64 MiB of HBM per device.

```python
import jax
import jax.numpy as jnp
from jax import lax

KVH = 8
HD = 128
G = 8
TOK_DEV = 128
QH = 64
SEQ_LEN = 1024
N_SEQ = 8


def base_keys(key):
    return jnp.clip(jax.random.normal(jax.random.fold_in(key, 3), (SEQ_LEN, KVH * HD), jnp.float32), -5.0, 5.0)


def draw_keys(key, part):
    drawn = base_keys(key)
    return drawn.astype(jnp.bfloat16)


def draw_queries(key, part):
    drawn = jnp.clip(jax.random.normal(jax.random.fold_in(key, 4), (SEQ_LEN, QH * HD), jnp.float32), -5.0, 5.0)
    return drawn.astype(jnp.bfloat16)


def block_levels(own_key, shape, cuts, low, top_value):
    factor_of = 1.0
    for axis_at, blocks in cuts:
        steps = jax.random.uniform(jax.random.fold_in(jax.random.fold_in(own_key, 6), axis_at), (blocks,), jnp.float32, low / len(cuts), top_value / len(cuts))
        factor_of = factor_of * jnp.repeat(jnp.exp(steps), shape[axis_at] // blocks).reshape((-1,) + (1,) * (len(shape) - 1 - axis_at))
    return factor_of


def scatter_about(key, extent, width, most, pieces=(), kind=jnp.bfloat16):
    result = jax.random.normal(key, extent, jnp.float32) * width
    if len(pieces) > 0:
        result = block_levels(key, extent, pieces, -0.22, 0.18) * result
    return jnp.clip(result, min=-most, max=most).astype(kind)


def setup_inputs(seed: int = 0) -> dict:
    arg_keys = jax.random.split(jax.random.key(seed), 9)
    return {
        "queries": draw_queries(jax.random.fold_in(arg_keys[8], 71), 0),
        "keys": draw_keys(jax.random.fold_in(arg_keys[8], 71), 0),
        "values": scatter_about(arg_keys[2], (SEQ_LEN, KVH * HD), 1.0, 6.0, ((0, 8), (1, 4))),
        "q_tangent": scatter_about(arg_keys[3], (SEQ_LEN, QH * HD), 1.0, 6.0, ((0, 8), (1, 4))),
        "k_tangent": scatter_about(arg_keys[4], (SEQ_LEN, KVH * HD), 1.0, 6.0, ((0, 8), (1, 4))),
        "v_tangent": scatter_about(arg_keys[5], (SEQ_LEN, KVH * HD), 1.0, 6.0, ((0, 8), (1, 4))),
        "out_grad": scatter_about(arg_keys[6], (SEQ_LEN, QH * HD), 1.0, 6.0, ((0, 8), (1, 4))),
        "block_order": jax.random.permutation(arg_keys[7], N_SEQ).astype(jnp.int32),
    }


neg_fill = -1e30


def rounded(value):
    return lax.optimization_barrier(value.astype(jnp.bfloat16)).astype(jnp.float32)


def reference(queries, keys, values, q_tangent, k_tangent, v_tangent, out_grad, block_order):
    scaling = HD ** -0.5
    positions = (block_order[:, None] * TOK_DEV + jnp.arange(TOK_DEV, dtype=jnp.int32)[None, :]).reshape(-1).astype(jnp.int32)
    key_full = keys.astype(jnp.float32).reshape(SEQ_LEN, KVH, HD)
    val_full = values.astype(jnp.float32).reshape(SEQ_LEN, KVH, HD)
    key_tan = k_tangent.astype(jnp.float32).reshape(SEQ_LEN, KVH, HD)
    val_tan = v_tangent.astype(jnp.float32).reshape(SEQ_LEN, KVH, HD)
    query_block = min(128, SEQ_LEN)
    block_total = SEQ_LEN // query_block

    def split_rows(array):
        return array.astype(jnp.float32).reshape(block_total, query_block, KVH, G, HD)

    inputs = (split_rows(queries), split_rows(q_tangent), split_rows(out_grad), positions.reshape(block_total, query_block))

    def one_block(carry, items):
        dk_acc, dv_acc = carry
        query_rows, query_tan, grad_rows, query_pos = items
        visible = (positions[None, :] <= query_pos[:, None])[None, None]
        s_main = jnp.einsum("thgd,shd->hgts", query_rows, key_full) * scaling
        s_tan = (jnp.einsum("thgd,shd->hgts", query_tan, key_full) + jnp.einsum("thgd,shd->hgts", query_rows, key_tan)) * scaling
        d_prob = jnp.einsum("thgd,shd->hgts", grad_rows, val_full)
        d_prob_tan = jnp.einsum("thgd,shd->hgts", grad_rows, val_tan)
        row_max = jnp.max(jnp.where(visible, s_main, neg_fill), axis=-1, keepdims=True)
        expo = jnp.where(visible, jnp.exp(s_main - row_max), 0.0)
        prob = expo / jnp.sum(expo, axis=-1, keepdims=True)
        tan_mean = jnp.sum(prob * s_tan, axis=-1, keepdims=True)
        prob_tan = prob * (s_tan - tan_mean)
        delta = jnp.sum(prob * d_prob, axis=-1, keepdims=True)
        delta_tan = jnp.sum(prob_tan * d_prob + prob * d_prob_tan, axis=-1, keepdims=True)
        d_score = prob * (d_prob - delta)
        d_score_tan = prob_tan * (d_prob - delta) + prob * (d_prob_tan - delta_tan)
        prob_tan_b = rounded(prob_tan)
        d_score_b = rounded(d_score)
        d_score_tan_b = rounded(d_score_tan)
        dq_part = (jnp.einsum("hgts,shd->thgd", d_score_tan_b, key_full) + jnp.einsum("hgts,shd->thgd", d_score_b, key_tan)) * scaling
        dk_part = (jnp.einsum("hgts,thgd->shd", d_score_tan_b, query_rows) + jnp.einsum("hgts,thgd->shd", d_score_b, query_tan)) * scaling
        dv_part = jnp.einsum("hgts,thgd->shd", prob_tan_b, grad_rows)
        return (dk_acc + dk_part, dv_acc + dv_part), dq_part

    empty = jnp.zeros((SEQ_LEN, KVH, HD), jnp.float32)
    (dk_total, dv_total), dq_blocks = lax.scan(one_block, (empty, empty), inputs)
    dq_tangent = dq_blocks.reshape(SEQ_LEN, QH * HD).astype(jnp.bfloat16)
    dk_tangent = dk_total.reshape(SEQ_LEN, KVH * HD).astype(jnp.bfloat16)
    dv_tangent = dv_total.reshape(SEQ_LEN, KVH * HD).astype(jnp.bfloat16)
    dq_wide = dq_tangent.astype(jnp.float32)
    dk_wide = dk_tangent.astype(jnp.float32)
    dv_wide = dv_tangent.astype(jnp.float32)
    squared_norm = jnp.sum(dq_wide * dq_wide) + jnp.sum(dk_wide * dk_wide) + jnp.sum(dv_wide * dv_wide)
    return dq_tangent, dk_tangent, dv_tangent, squared_norm
```

```python
import functools

import jax
import jax.numpy as jnp
from jax import lax
from jax.experimental import pallas as pl
from jax.experimental.pallas import tpu as pltpu
from jax.sharding import PartitionSpec as P

HD = 128
G = 8
ROWS = 256
CHUNK = 256
LOG2E = 1.4426950408889634
FILL = -1e30

NT = (((1,), (1,)), ((), ()))
NN = (((1,), (0,)), ((), ()))


def dot(a, b, dims):
    return lax.dot_general(a, b, dims, preferred_element_type=jnp.float32)


def hvp_kernel(
    seq_of, n_kv, tokens, width, col_of, scaling,
    me_ref, order_ref, q_ref, qt_ref, do_ref, peer_ref, *rest
):
    kv_refs = rest[:n_kv]
    dq_own_ref, dq_peer_ref = rest[n_kv : n_kv + 2]
    out_refs = rest[n_kv + 2 : 2 * n_kv + 2]
    (qs, kvs, kts, e_s, st_s, dp_s, dpt_s, mc_s, dq_acc, acc, sem) = rest[2 * n_kv + 2 :]
    groups = width // HD
    tiles = width // ROWS
    per_tile = ROWS // tokens
    me = me_ref[0]
    first = col_of(me)

    copies = []
    for which, ref in enumerate((q_ref, qt_ref, do_ref)):
        for g in range(groups):
            copies.append(
                pltpu.make_async_copy(
                    ref.at[:, pl.ds(pl.multiple_of(first + g * HD, HD), HD)],
                    qs.at[0, g // per_tile, which, pl.ds((g % per_tile) * tokens, tokens), :],
                    sem.at[0],
                )
            )
            copies.append(
                pltpu.make_async_copy(
                    peer_ref.at[:, pl.ds(which * width + g * HD, HD)],
                    qs.at[1, g // per_tile, which, pl.ds((g % per_tile) * tokens, tokens), :],
                    sem.at[0],
                )
            )
    for m, ref in enumerate(kv_refs):
        for e in range(ref.shape[0]):
            copies.append(
                pltpu.make_async_copy(
                    ref.at[e], kvs.at[order_ref[seq_of(me, m, e)]], sem.at[0]
                )
            )
    for c in copies:
        c.start()
    acc[...] = jnp.zeros_like(acc)
    for c in copies:
        c.wait()

    blocks = kvs.shape[0]
    per_chunk = CHUNK // tokens
    chunks = blocks // per_chunk

    def chunk_kv(kc):
        return kvs[pl.ds(kc * per_chunk, per_chunk)].reshape(CHUNK, 4 * HD)

    def transpose_keys(kc, _):
        kv = chunk_kv(kc)
        kts[kc] = jnp.concatenate([kv[:, :HD].T, kv[:, HD : 2 * HD].T], axis=1)
        return 0

    lax.fori_loop(0, chunks, transpose_keys, 0)

    scale2 = scaling * LOG2E
    key_iota = lax.broadcasted_iota(jnp.int32, (CHUNK, ROWS), 0)
    row_iota = lax.rem(lax.broadcasted_iota(jnp.int32, (CHUNK, ROWS), 1), tokens)
    behind = row_iota - key_iota

    def split(x):
        return x.reshape(x.shape[0] // 8, 8, x.shape[1])

    def tile(r, _):
        i = r // tiles
        t = lax.rem(r, tiles)
        b = order_ref[jnp.where(i == 0, me, me ^ 1)]
        q = qs[i, t, 0]
        qt = qs[i, t, 1]
        do = qs[i, t, 2]
        qq = jnp.concatenate([qt, q], axis=1)
        full = (b * tokens) // CHUNK

        def scores(kc, stats, masked):
            m_old, z, s1, d1, x1, y1 = stats
            kv = chunk_kv(kc)
            s = dot(kv[:, :HD], q, NT)
            if masked:
                s = jnp.where(behind >= kc * CHUNK - b * tokens, s, FILL)
            st = dot(kv[:, : 2 * HD], qq, NT)
            dp = dot(kv[:, 2 * HD : 3 * HD], do, NT)
            dpt = dot(kv[:, 3 * HD :], do, NT)
            st_s[kc] = st
            dp_s[kc] = dp
            dpt_s[kc] = dpt
            s = split(s) * scale2
            m_new = jnp.maximum(m_old, jnp.max(s, axis=0))
            decay = jnp.exp2(m_old - m_new)
            e = jnp.exp2(s - m_new[None])
            e_s[kc] = e.reshape(CHUNK, ROWS)
            mc_s[kc] = m_new
            est = e * split(st)
            dp3 = split(dp)
            return (
                m_new,
                z * decay + jnp.sum(e, axis=0),
                s1 * decay + jnp.sum(est, axis=0),
                d1 * decay + jnp.sum(e * dp3, axis=0),
                x1 * decay + jnp.sum(est * dp3, axis=0),
                y1 * decay + jnp.sum(e * split(dpt), axis=0),
            )

        zero = jnp.zeros((8, ROWS), jnp.float32)
        start = (jnp.full((8, ROWS), FILL, jnp.float32), zero, zero, zero, zero, zero)
        stats = lax.fori_loop(0, full, functools.partial(scores, masked=False), start)
        m8, z, s1, d1, x1, y1 = scores(full, stats, True)
        top = jnp.max(m8, axis=0, keepdims=True)
        w8 = jnp.exp2(m8 - top)

        def total(v):
            return jnp.sum(v * w8, axis=0, keepdims=True)

        rz = 1.0 / total(z)
        tan_mean = total(s1) * rz
        delta = total(d1) * rz
        delta_tan = scaling * (total(x1) * rz - tan_mean * delta) + total(y1) * rz
        dq_acc[...] = jnp.zeros_like(dq_acc)

        def grads(kc, _):
            f = jnp.exp2(mc_s[kc] - top) * rz
            e = split(e_s[kc])
            p = e * f[None]
            pt = e * (f * scaling)[None] * (split(st_s[kc]) - tan_mean[None])
            dd = split(dp_s[kc]) - delta[None]
            ds = (p * dd).reshape(CHUNK, ROWS).astype(jnp.bfloat16)
            dst = (pt * dd + p * (split(dpt_s[kc]) - delta_tan[None])).reshape(CHUNK, ROWS)
            dst = dst.astype(jnp.bfloat16)
            pt = pt.reshape(CHUNK, ROWS).astype(jnp.bfloat16)
            dq_acc[...] += dot(kts[kc], jnp.concatenate([dst, ds], axis=0), NN)
            dk = dot(
                jnp.concatenate([dst, ds], axis=1), jnp.concatenate([q, qt], axis=0), NN
            )
            dv = dot(pt, do, NN)
            at = pl.ds(kc * per_chunk, per_chunk)
            acc[at] += jnp.concatenate([dk, dv], axis=1).reshape(per_chunk, tokens, 2 * HD)
            return 0

        lax.fori_loop(0, full + 1, grads, 0)
        dq = (dq_acc[...] * scaling).T.astype(jnp.bfloat16)
        for h in range(per_tile):
            part = dq[h * tokens : (h + 1) * tokens]
            cols = pl.ds(pl.multiple_of((t * per_tile + h) * HD, HD), HD)

            @pl.when(i == 0)
            def _():
                dq_own_ref[:, cols] = part

            @pl.when(i == 1)
            def _():
                dq_peer_ref[:, cols] = part

        return 0

    lax.fori_loop(0, 2 * tiles, tile, 0)

    for m, ref in enumerate(out_refs):

        def store(e, _, ref=ref, m=m):
            block = acc[order_ref[seq_of(me, m, e)]]
            ref[e, :, :HD] = (block[:, :HD] * scaling).astype(ref.dtype)
            ref[e, :, HD:] = block[:, HD:].astype(ref.dtype)
            return 0

        lax.fori_loop(0, ref.shape[0], store, 0)


def run_hvp(me, order, q, qt, do, peer, kvs, out_dtypes, seq_of, col_of, width):
    tokens = q.shape[0]
    blocks = sum(k.shape[0] for k in kvs)
    chunks = blocks * tokens // CHUNK
    tiles = width // ROWS
    f32 = jnp.float32
    score = pltpu.VMEM((chunks, CHUNK, ROWS), f32)
    kernel = functools.partial(
        hvp_kernel, seq_of, len(kvs), tokens, width, col_of, HD ** (-0.5)
    )
    outs = [jax.ShapeDtypeStruct((tokens, width), jnp.bfloat16)] * 2 + [
        jax.ShapeDtypeStruct(k.shape[:2] + (2 * HD,), d) for k, d in zip(kvs, out_dtypes)
    ]
    flops = 2 * blocks * tokens * tokens * width * 10
    return pl.pallas_call(
        kernel,
        name="hvp",
        out_shape=outs,
        in_specs=[pl.BlockSpec(memory_space=pltpu.SMEM)] * 2
        + [pl.BlockSpec(memory_space=pl.ANY)] * (4 + len(kvs)),
        out_specs=[pl.BlockSpec(memory_space=pltpu.VMEM)] * len(outs),
        scratch_shapes=[
            pltpu.VMEM((2, tiles, 3, ROWS, HD), jnp.bfloat16),
            pltpu.VMEM((blocks, tokens, 4 * HD), jnp.bfloat16),
            pltpu.VMEM((chunks, HD, 2 * CHUNK), jnp.bfloat16),
            score,
            score,
            score,
            score,
            pltpu.VMEM((chunks, 8, ROWS), f32),
            pltpu.VMEM((HD, ROWS), f32),
            pltpu.VMEM((blocks, tokens, 2 * HD), f32),
            pltpu.SemaphoreType.DMA((1,)),
        ],
        compiler_params=pltpu.CompilerParams(vmem_limit_bytes=48 * 1024 * 1024),
        cost_estimate=pl.CostEstimate(flops=flops, bytes_accessed=4 << 20, transcendentals=0),
    )(me, order, q, qt, do, peer, *kvs)


def shifted(x, axis, bit):
    size = lax.axis_size(axis)
    return lax.ppermute(x, axis, [(i, i ^ bit) for i in range(size)])


def all_sum(x, axes):
    for axis in axes:
        size = lax.axis_size(axis)
        if size & (size - 1):
            x = lax.psum(x, axis)
            continue
        bit = 1
        while bit < size:
            x = x + shifted(x, axis, bit)
            bit *= 2
    return x


def square_sum(x):
    w = x.astype(jnp.float32)
    return jnp.sum(w * w)


def join(core, mine, theirs):
    low = jnp.where(core == 0, mine, theirs)
    high = jnp.where(core == 0, theirs, mine)
    return jnp.concatenate([low, high], axis=1)


def body(queries, keys, values, q_tangent, k_tangent, v_tangent, out_grad, block_order):
    tokens = queries.shape[0]
    heads = keys.shape[1] // HD
    shards = lax.axis_size("seq")
    me = lax.axis_index("seq").astype(jnp.int32)
    core = lax.rem(me, 2)
    me_arr = me.reshape(1)
    width = heads * G * HD // 2
    other = (1 - core) * width
    f32 = jnp.float32

    peer_rows = jnp.concatenate(
        [
            lax.dynamic_slice_in_dim(x, other, width, 1)
            for x in (queries, q_tangent, out_grad)
        ],
        axis=1,
    )
    peer_rows = shifted(peer_rows, "seq", 1)

    def col_of(at):
        return lax.rem(at, 2) * width

    def pack(head):
        return jnp.concatenate(
            [
                lax.dynamic_slice_in_dim(x, head * HD, HD, 1)
                for x in (keys, k_tangent, values, v_tangent)
            ],
            axis=1,
        )

    if heads == 2 and shards == 8:
        mine = pack(core)
        theirs = shifted(pack(1 - core), "seq", 1)
        chip = jnp.stack([mine, theirs])
        x_kv = shifted(chip, "seq", 2)
        y_kv = shifted(chip, "seq", 4)
        half = 2 * HD
        xy_a = shifted(y_kv[:, :, :half], "seq", 2)
        xy_b = shifted(x_kv[:, :, half:], "seq", 4)
        xy_kv = jnp.concatenate([xy_a, xy_b], axis=2)
        dq_own, dq_peer, own, to_x, to_y, to_xy = run_hvp(
            me_arr, block_order, queries, q_tangent, out_grad, peer_rows,
            (chip, x_kv, y_kv, xy_kv),
            (f32, jnp.bfloat16, jnp.bfloat16, jnp.bfloat16),
            lambda at, m, e: at ^ (2 * m + e), col_of, width,
        )
        got = (shifted(to_x, "seq", 2), shifted(to_y, "seq", 4), shifted(to_xy, "seq", 6))
        final = (own + sum(g.astype(f32) for g in got)).astype(jnp.bfloat16)
        local = square_sum(final)
        back = shifted(final[1], "seq", 1)
        dk_out = join(core, final[0][:, :HD], back[:, :HD])
        dv_out = join(core, final[0][:, HD:], back[:, HD:])
    else:
        whole = lax.all_gather(pack(0), "seq", axis=0)
        dq_own, dq_peer, parts = run_hvp(
            me_arr, block_order, queries, q_tangent, out_grad, peer_rows,
            (whole,), (jnp.bfloat16,), lambda at, m, e: e, col_of, width,
        )
        final = lax.psum_scatter(parts, "seq", scatter_dimension=0)
        local = square_sum(final)
        dk_out = final[:, :HD]
        dv_out = final[:, HD:]
    local = local + square_sum(dq_own) + square_sum(dq_peer)
    dq_out = join(core, dq_own, shifted(dq_peer, "seq", 1))
    squared_norm = all_sum(local, ("seq", "head"))
    return (dq_out, dk_out, dv_out, squared_norm)


def solution(mesh):
    placed = (P("seq", "head"),) * 7 + (P(),)
    return jax.shard_map(
        body,
        mesh=mesh,
        in_specs=placed,
        out_specs=(P("seq", "head"), P("seq", "head"), P("seq", "head"), P()),
        check_vma=False,
    )
```

```python
import functools

import jax
import jax.numpy as jnp
from jax import lax
from jax.experimental import pallas as pl
from jax.experimental.pallas import tpu as pltpu
from jax.sharding import PartitionSpec as P

HD = 128
G = 8
ROWS = 256
CHUNK = 256
LOG2E = 1.4426950408889634
FILL = -1e30

NT = (((1,), (1,)), ((), ()))
NN = (((1,), (0,)), ((), ()))


def dot(a, b, dims):
    return lax.dot_general(a, b, dims, preferred_element_type=jnp.float32)


def hvp_kernel(
    seq_of, out_seq, n_kv, n_out, tokens, width, col_of, scaling,
    me_ref, order_ref, q_ref, qt_ref, do_ref, peer_ref, *rest
):
    kv_refs = rest[:n_kv]
    dq_ref, sq_ref = rest[n_kv : n_kv + 2]
    out_refs = rest[n_kv + 2 : n_kv + 2 + n_out]
    rest = rest[n_kv + 2 + n_out :]
    (qs, kvs, kts, x_s, dq_acc, acc, sem, mc_a, mc_b) = rest[:9]
    slot_a, slot_b = rest[9:13], rest[13:]
    groups = width // HD
    tiles = width // ROWS
    per_tile = ROWS // tokens
    me = me_ref[0]
    first = col_of(me)

    copies = []
    for which, ref in enumerate((q_ref, qt_ref, do_ref)):
        for g in range(groups):
            copies.append(
                pltpu.make_async_copy(
                    ref.at[:, pl.ds(pl.multiple_of(first + g * HD, HD), HD)],
                    qs.at[0, g // per_tile, which, pl.ds((g % per_tile) * tokens, tokens), :],
                    sem.at[0],
                )
            )
            copies.append(
                pltpu.make_async_copy(
                    peer_ref.at[:, pl.ds(which * width + g * HD, HD)],
                    qs.at[1, g // per_tile, which, pl.ds((g % per_tile) * tokens, tokens), :],
                    sem.at[0],
                )
            )
    for m, ref in enumerate(kv_refs):
        for e in range(ref.shape[0]):
            copies.append(
                pltpu.make_async_copy(
                    ref.at[e], kvs.at[order_ref[seq_of(me, m, e)]], sem.at[0]
                )
            )
    for c in copies:
        c.start()
    acc[...] = jnp.zeros_like(acc)
    sq_ref[...] = jnp.zeros_like(sq_ref)
    for c in copies:
        c.wait()

    blocks = kvs.shape[0]
    per_chunk = CHUNK // tokens
    chunks = blocks // per_chunk

    def chunk_kv(kc):
        return kvs[pl.ds(kc * per_chunk, per_chunk)].reshape(CHUNK, 4 * HD)

    def transpose_keys(kc, _):
        kv = chunk_kv(kc)
        kts[kc] = jnp.concatenate([kv[:, :HD].T, kv[:, HD : 2 * HD].T], axis=1)
        return 0

    lax.fori_loop(0, chunks, transpose_keys, 0)

    scale2 = scaling * LOG2E
    key_iota = lax.broadcasted_iota(jnp.int32, (CHUNK, ROWS), 0)
    row_iota = lax.rem(lax.broadcasted_iota(jnp.int32, (CHUNK, ROWS), 1), tokens)
    behind = row_iota - key_iota

    def split(x):
        return x.reshape(x.shape[0] // 8, 8, x.shape[1])

    piece = 32

    def score_dots(t_rows, slot, kc, masked, b):
        q, qt, do = t_rows
        s_s, st_s, dp_s, dpt_s = slot
        kv = chunk_kv(kc)
        s = dot(kv[:, :HD], q, NT)
        if masked:
            s = jnp.where(behind >= kc * CHUNK - b * tokens, s, FILL)
        s_s[kc] = s
        st_s[kc] = dot(kv[:, : 2 * HD], jnp.concatenate([qt, q], axis=1), NT)
        dp_s[kc] = dot(kv[:, 2 * HD : 3 * HD], do, NT)
        dpt_s[kc] = dot(kv[:, 3 * HD :], do, NT)

    def score_sums(slot, mc_s, kc, stats):
        s_s, st_s, dp_s, dpt_s = slot
        m_old, z, s1, d1, x1, y1 = stats
        m_new = m_old
        for k in range(0, CHUNK, piece):
            s = split(s_s[kc, k : k + piece])
            m_new = jnp.maximum(m_new, jnp.max(s, axis=0) * scale2)
        decay = jnp.exp2(m_old - m_new)
        mc_s[kc] = m_new
        z, s1, d1, x1, y1 = [v * decay for v in (z, s1, d1, x1, y1)]
        for k in range(0, CHUNK, piece):
            at = slice(k, k + piece)
            e = jnp.exp2(split(s_s[kc, at]) * scale2 - m_new[None])
            s_s[kc, at] = e.reshape(piece, ROWS)
            est = e * split(st_s[kc, at])
            dp = split(dp_s[kc, at])
            z = z + jnp.sum(e, axis=0)
            s1 = s1 + jnp.sum(est, axis=0)
            d1 = d1 + jnp.sum(e * dp, axis=0)
            x1 = x1 + jnp.sum(est * dp, axis=0)
            y1 = y1 + jnp.sum(e * split(dpt_s[kc, at]), axis=0)
        return (m_new, z, s1, d1, x1, y1)

    def finish(stats):
        m8, z, s1, d1, x1, y1 = stats
        top = jnp.max(m8, axis=0, keepdims=True)
        w8 = jnp.exp2(m8 - top)

        def total(v):
            return jnp.sum(v * w8, axis=0, keepdims=True)

        rz = 1.0 / total(z)
        tan_mean = total(s1) * rz
        delta = total(d1) * rz
        delta_tan = scaling * (total(x1) * rz - tan_mean * delta) + total(y1) * rz
        return (top, rz, tan_mean, delta, delta_tan)

    def grad_values(slot, mc_s, kc, done):
        s_s, st_s, dp_s, dpt_s = slot
        top, rz, tan_mean, delta, delta_tan = done
        f = jnp.exp2(mc_s[kc] - top) * rz
        fc = f * scaling
        for k in range(0, CHUNK, piece):
            at = slice(k, k + piece)
            e = split(s_s[kc, at])
            p = e * f[None]
            pt = e * fc[None] * (split(st_s[kc, at]) - tan_mean[None])
            dd = split(dp_s[kc, at]) - delta[None]
            dst = pt * dd + p * (split(dpt_s[kc, at]) - delta_tan[None])
            for j, v in enumerate((dst, p * dd, pt)):
                x_s[j, at] = v.reshape(piece, ROWS).astype(jnp.bfloat16)

    def grad_dots(t_rows, kc):
        q, qt, do = t_rows
        dst, ds, pt = x_s[0], x_s[1], x_s[2]
        dq_acc[...] += dot(kts[kc], jnp.concatenate([dst, ds], axis=0), NN)
        dk = dot(jnp.concatenate([dst, ds], axis=1), jnp.concatenate([q, qt], axis=0), NN)
        dv = dot(pt, do, NN)
        at = pl.ds(kc * per_chunk, per_chunk)
        acc[at] += jnp.concatenate([dk, dv], axis=1).reshape(per_chunk, tokens, 2 * HD)

    slots = (slot_a, slot_b)
    mcs = (mc_a, mc_b)
    zero = jnp.zeros((8, ROWS), jnp.float32)
    start = (jnp.full((8, ROWS), FILL, jnp.float32), zero, zero, zero, zero, zero)

    def block(i, _):
        b = order_ref[jnp.where(i == 0, me, me ^ 1)]
        full = (b * tokens) // CHUNK

        def rows(t):
            return (qs[i, t, 0], qs[i, t, 1], qs[i, t, 2])

        def step(kc, stats, t, done, masked):
            now, nxt = t % 2, (t + 1) % 2
            if done is not None:
                grad_values(slots[now], mcs[now], kc, done)
            if t + 1 < tiles:
                score_dots(rows(t + 1), slots[nxt], kc, masked, b)
            if done is not None:
                grad_dots(rows(t), kc)
            if t + 1 < tiles:
                stats = score_sums(slots[nxt], mcs[nxt], kc, stats)
            return stats

        done = None
        for t in range(-1, tiles):
            if done is not None:
                dq_acc[...] = jnp.zeros_like(dq_acc)
            if t + 1 < tiles:
                stats = lax.fori_loop(
                    0, full, functools.partial(step, t=t, done=done, masked=False), start
                )
                stats = step(full, stats, t, done, True)
            else:
                stats = lax.fori_loop(
                    0, full + 1, functools.partial(step, t=t, done=done, masked=False), start
                )
            if done is not None:
                dq = (dq_acc[...] * scaling).T.astype(jnp.bfloat16)
                wide = dq.astype(jnp.float32)
                sq_ref[...] += jnp.sum(split(wide * wide), axis=0)
                for h in range(per_tile):
                    part = dq[h * tokens : (h + 1) * tokens]
                    c = (t * per_tile + h) * HD
                    dq_ref[i, :, c : c + HD] = part
            done = finish(stats)
        return 0

    lax.fori_loop(0, 2, block, 0)

    for m, ref in enumerate(out_refs):
        for e in range(ref.shape[0] // tokens):
            block_at = acc[order_ref[out_seq(me, m, e)]]
            rows_at = slice(e * tokens, (e + 1) * tokens)
            ref[rows_at, :HD] = (block_at[:, :HD] * scaling).astype(ref.dtype)
            ref[rows_at, HD:] = block_at[:, HD:].astype(ref.dtype)


def run_hvp(me, order, q, qt, do, peer, kvs, outs, seq_of, out_seq, col_of, width):
    tokens = q.shape[0]
    blocks = sum(k.shape[0] for k in kvs)
    chunks = blocks * tokens // CHUNK
    tiles = width // ROWS
    f32 = jnp.float32
    score = pltpu.VMEM((chunks, CHUNK, ROWS), f32)
    kernel = functools.partial(
        hvp_kernel, seq_of, out_seq, len(kvs), len(outs), tokens, width, col_of, HD ** (-0.5)
    )
    outs = [
        jax.ShapeDtypeStruct((2, tokens, width), jnp.bfloat16),
        jax.ShapeDtypeStruct((8, HD), f32),
    ] + outs
    flops = 2 * blocks * tokens * tokens * width * 10
    return pl.pallas_call(
        kernel,
        name="hvp",
        out_shape=outs,
        in_specs=[pl.BlockSpec(memory_space=pltpu.SMEM)] * 2
        + [pl.BlockSpec(memory_space=pl.ANY)] * (4 + len(kvs)),
        out_specs=[pl.BlockSpec(memory_space=pltpu.VMEM)] * len(outs),
        scratch_shapes=[
            pltpu.VMEM((2, tiles, 3, ROWS, HD), jnp.bfloat16),
            pltpu.VMEM((blocks, tokens, 4 * HD), jnp.bfloat16),
            pltpu.VMEM((chunks, HD, 2 * CHUNK), jnp.bfloat16),
            pltpu.VMEM((3, CHUNK, ROWS), jnp.bfloat16),
            pltpu.VMEM((HD, ROWS), f32),
            pltpu.VMEM((blocks, tokens, 2 * HD), f32),
            pltpu.SemaphoreType.DMA((1,)),
            pltpu.VMEM((chunks, 8, ROWS), f32),
            pltpu.VMEM((chunks, 8, ROWS), f32),
        ]
        + [score] * 8,
        compiler_params=pltpu.CompilerParams(vmem_limit_bytes=48 * 1024 * 1024),
        cost_estimate=pl.CostEstimate(flops=flops, bytes_accessed=4 << 20, transcendentals=0),
    )(me, order, q, qt, do, peer, *kvs)


def join_kernel(copies, me_ref, own_ref, *rest):
    got = rest[: copies - 1]
    dq_ref, dq_got_ref, sq_ref, dq_out, dk_out, dv_out, sum_ref, sem = rest[copies - 1 :]
    width = dq_ref.shape[2]
    core = lax.rem(me_ref[0], 2)
    mine = pl.multiple_of(core * width, HD)
    theirs = pl.multiple_of((1 - core) * width, HD)
    moves = (
        pltpu.make_async_copy(dq_ref.at[0], dq_out.at[:, pl.ds(mine, width)], sem.at[0]),
        pltpu.make_async_copy(dq_got_ref, dq_out.at[:, pl.ds(theirs, width)], sem.at[1]),
    )
    for move in moves:
        move.start()
    f32 = jnp.float32
    total = sq_ref[...]
    for side in range(2):
        at = pl.ds(pl.multiple_of((core if side == 0 else 1 - core) * HD, HD), HD)
        for half, out in enumerate((dk_out, dv_out)):
            cols = slice(half * HD, (half + 1) * HD)
            parts = [got[m - 1][:, cols].astype(f32) for m in range(2 - side, copies, 2)]
            if side == 0:
                parts = [own_ref[:, cols]] + parts
            final = sum(parts[1:], parts[0]).astype(jnp.bfloat16)
            out[:, at] = final
            wide = final.astype(f32)
            total = total + jnp.sum((wide * wide).reshape(-1, 8, HD), axis=0)
    line = jnp.sum(total, axis=0, keepdims=True)
    sum_ref[...] = jnp.broadcast_to(line[None], sum_ref.shape)
    for move in moves:
        move.wait()


def run_join(me, own, got, dq, dq_got, sq, devices):
    tokens, cols = own.shape
    width = dq.shape[2]
    half = jax.ShapeDtypeStruct((tokens, 2 * HD), jnp.bfloat16)
    return pl.pallas_call(
        functools.partial(join_kernel, len(got) + 1),
        name="join",
        out_shape=[
            jax.ShapeDtypeStruct((tokens, 2 * width), jnp.bfloat16),
            half,
            half,
            jax.ShapeDtypeStruct((devices, 1, HD), jnp.float32),
        ],
        in_specs=[pl.BlockSpec(memory_space=pltpu.SMEM)]
        + [pl.BlockSpec(memory_space=pltpu.VMEM)] * (len(got) + 4),
        out_specs=[pl.BlockSpec(memory_space=pl.ANY)]
        + [pl.BlockSpec(memory_space=pltpu.VMEM)] * 3,
        scratch_shapes=[pltpu.SemaphoreType.DMA((2,))],
        cost_estimate=pl.CostEstimate(flops=1 << 20, bytes_accessed=2 << 20, transcendentals=0),
    )(me, own, *got, dq, dq_got, sq)


def shifted(x, axis, bit):
    size = lax.axis_size(axis)
    return lax.ppermute(x, axis, [(i, i ^ bit) for i in range(size)])


def all_sum(x, axes):
    for axis in axes:
        size = lax.axis_size(axis)
        if size & (size - 1):
            x = lax.psum(x, axis)
            continue
        bit = 1
        while bit < size:
            x = x + shifted(x, axis, bit)
            bit *= 2
    return x


def square_sum(x):
    w = x.astype(jnp.float32)
    return jnp.sum(w * w)


def join(core, mine, theirs):
    low = jnp.where(core == 0, mine, theirs)
    high = jnp.where(core == 0, theirs, mine)
    return jnp.concatenate([low, high], axis=1)


def body(queries, keys, values, q_tangent, k_tangent, v_tangent, out_grad, block_order):
    tokens = queries.shape[0]
    heads = keys.shape[1] // HD
    shards = lax.axis_size("seq")
    me = lax.axis_index("seq").astype(jnp.int32)
    core = lax.rem(me, 2)
    me_arr = me.reshape(1)
    width = heads * G * HD // 2
    other = (1 - core) * width
    f32 = jnp.float32

    def swap_rows(arrays):
        cut = [lax.dynamic_slice_in_dim(x, other, width, 1) for x in arrays]
        return shifted(jnp.concatenate(cut, axis=1), "seq", 1)

    rows = (queries, q_tangent, out_grad)

    def col_of(at):
        return lax.rem(at, 2) * width

    def pack(head):
        return jnp.concatenate(
            [
                lax.dynamic_slice_in_dim(x, head * HD, HD, 1)
                for x in (keys, k_tangent, values, v_tangent)
            ],
            axis=1,
        )

    if heads == 2 and shards == 8:
        mine = pack(core)
        theirs = shifted(pack(1 - core), "seq", 1)
        chip = jnp.stack([mine, theirs])
        *late, _ = lax.optimization_barrier((*rows, theirs))
        x_kv = shifted(chip, "seq", 2)
        y_kv = shifted(chip, "seq", 4)
        peer_rows = swap_rows(late)
        half = 2 * HD
        xy_a = shifted(y_kv[:, :, :half], "seq", 2)
        xy_b = shifted(x_kv[:, :, half:], "seq", 4)
        xy_kv = jnp.concatenate([xy_a, xy_b], axis=2)
        dq, sq, own, *parts = run_hvp(
            me_arr, block_order, *rows, peer_rows, (chip, x_kv, y_kv, xy_kv),
            [jax.ShapeDtypeStruct((tokens, 2 * HD), f32)]
            + [jax.ShapeDtypeStruct((tokens, 2 * HD), jnp.bfloat16)] * (shards - 1),
            lambda at, m, e: at ^ (2 * m + e), lambda at, m, e: at ^ m, col_of, width,
        )
        got = [shifted(p, "seq", m + 1) for m, p in enumerate(parts)]
        dq_got = shifted(dq[1], "seq", 1)
        devices = shards * lax.axis_size("head")
        dq_out, dk_out, dv_out, line = run_join(me_arr, own, got, dq, dq_got, sq, devices)
        line = lax.all_to_all(line, ("head", "seq"), 0, 0)
        return (dq_out, dk_out, dv_out, jnp.sum(line))
    assert heads == 1
    whole = lax.all_gather(pack(0), "seq", axis=0)
    dq, sq, parts = run_hvp(
        me_arr, block_order, *rows, swap_rows(rows), (whole,),
        [jax.ShapeDtypeStruct((shards * tokens, 2 * HD), jnp.bfloat16)],
        lambda at, m, e: e, lambda at, m, e: e, col_of, width,
    )
    final = lax.psum_scatter(parts, "seq", scatter_dimension=0, tiled=True)
    dq_out = join(core, dq[0], shifted(dq[1], "seq", 1))
    local = square_sum(final) + jnp.sum(sq)
    squared_norm = all_sum(local, ("seq", "head"))
    return (dq_out, final[:, :HD], final[:, HD:], squared_norm)


def solution(mesh):
    placed = (P("seq", "head"),) * 7 + (P(),)
    return jax.shard_map(
        body,
        mesh=mesh,
        in_specs=placed,
        out_specs=(P("seq", "head"), P("seq", "head"), P("seq", "head"), P()),
        check_vma=False,
    )
```

```python
import functools

import jax
import jax.numpy as jnp
from jax import lax
from jax.experimental import pallas as pl
from jax.experimental.pallas import tpu as pltpu
from jax.sharding import PartitionSpec as P

HD = 128
G = 8
ROWS = 256
CHUNK = 256
LOG2E = 1.4426950408889634
FILL = -1e30

NT = (((1,), (1,)), ((), ()))
NN = (((1,), (0,)), ((), ()))


def dot(a, b, dims):
    return lax.dot_general(a, b, dims, preferred_element_type=jnp.float32)


def hvp_kernel(
    seq_of, out_seq, n_own, n_kv, n_out, tokens, width, col_of, scaling,
    me_ref, order_hbm, q_ref, qt_ref, do_ref, peer_ref, *rest
):
    own_kv, rest = rest[:n_own], rest[n_own:]
    kv_refs = rest[:n_kv]
    dq_ref, sq_ref = rest[n_kv : n_kv + 2]
    out_refs = rest[n_kv + 2 : n_kv + 2 + n_out]
    rest = rest[n_kv + 2 + n_out :]
    groups = width // HD
    tiles = width // ROWS
    qs, kvs, kts, acc, sem, stats, order_ref = rest[:7]
    mcs, dqs, xs = (rest[7 + j * tiles : 7 + (j + 1) * tiles] for j in range(3))
    scores = [rest[7 + 3 * tiles + 4 * t :][:4] for t in range(tiles)]
    per_tile = ROWS // tokens
    me = me_ref[0]
    first = col_of(me)

    table = pltpu.make_async_copy(order_hbm, order_ref, sem.at[1])
    table.start()
    copies = []
    for which, ref in enumerate((q_ref, qt_ref, do_ref)):
        for g in range(groups):
            copies.append(
                pltpu.make_async_copy(
                    ref.at[:, pl.ds(pl.multiple_of(first + g * HD, HD), HD)],
                    qs.at[0, g // per_tile, which, pl.ds((g % per_tile) * tokens, tokens), :],
                    sem.at[0],
                )
            )
            copies.append(
                pltpu.make_async_copy(
                    peer_ref.at[:, pl.ds(which * width + g * HD, HD)],
                    qs.at[1, g // per_tile, which, pl.ds((g % per_tile) * tokens, tokens), :],
                    sem.at[0],
                )
            )
    for c in copies:
        c.start()
    table.wait()
    late = []
    for j, ref in enumerate(own_kv):
        head = pl.ds(pl.multiple_of(lax.rem(me, 2) * HD, HD), HD)
        to = kvs.at[order_ref[me], :, pl.ds(j * HD, HD)]
        late.append(pltpu.make_async_copy(ref.at[:, head], to, sem.at[0]))
    for m, ref in enumerate(kv_refs):
        for e in range(ref.shape[0]):
            at = order_ref[seq_of(me, m, e)]
            late.append(pltpu.make_async_copy(ref.at[e], kvs.at[at], sem.at[0]))
    for c in late:
        c.start()
    copies += late
    acc[...] = jnp.zeros_like(acc)
    sq_ref[...] = jnp.zeros_like(sq_ref)
    for c in copies:
        c.wait()

    blocks = kvs.shape[0]
    per_chunk = CHUNK // tokens
    chunks = blocks // per_chunk

    def chunk_kv(kc):
        return kvs[pl.ds(kc * per_chunk, per_chunk)].reshape(CHUNK, 4 * HD)

    def transpose_keys(kc, _):
        kv = chunk_kv(kc)
        kts[kc] = jnp.concatenate([kv[:, :HD].T, kv[:, HD : 2 * HD].T], axis=1)
        return 0

    lax.fori_loop(0, chunks, transpose_keys, 0)

    scale2 = scaling * LOG2E
    key_iota = lax.broadcasted_iota(jnp.int32, (CHUNK, ROWS), 0)
    row_iota = lax.rem(lax.broadcasted_iota(jnp.int32, (CHUNK, ROWS), 1), tokens)
    behind = row_iota - key_iota

    def split(x):
        return x.reshape(x.shape[0] // 8, 8, x.shape[1])

    piece = 32
    span = min(1, tiles)

    def score_dots(i, t, kc, masked, b):
        s_s, st_s, dp_s, dpt_s = scores[t]
        q, qt, do = qs[i, t, 0], qs[i, t, 1], qs[i, t, 2]
        kv = chunk_kv(kc)
        s = dot(kv[:, :HD], q, NT)
        if masked:
            s = jnp.where(behind >= kc * CHUNK - b * tokens, s, FILL)
        s_s[kc] = s
        st_s[kc] = dot(kv[:, : 2 * HD], jnp.concatenate([qt, q], axis=1), NT)
        both = dot(
            jnp.concatenate([kv[:, 2 * HD : 3 * HD], kv[:, 3 * HD :]], axis=0), do, NT
        )
        dp_s[kc] = both[:CHUNK]
        dpt_s[kc] = both[CHUNK:]

    def score_sums(t, kc):
        s_s, st_s, dp_s, dpt_s = scores[t]
        m_old, z, s1, d1, x1, y1 = [stats[t, j] for j in range(6)]
        m_new = m_old
        for k in range(0, CHUNK, piece):
            s = split(s_s[kc, k : k + piece])
            m_new = jnp.maximum(m_new, jnp.max(s, axis=0) * scale2)
        decay = jnp.exp2(m_old - m_new)
        mcs[t][kc] = m_new
        z, s1, d1, x1, y1 = [v * decay for v in (z, s1, d1, x1, y1)]
        for k in range(0, CHUNK, piece):
            at = slice(k, k + piece)
            e = jnp.exp2(split(s_s[kc, at]) * scale2 - m_new[None])
            s_s[kc, at] = e.reshape(piece, ROWS)
            est = e * split(st_s[kc, at])
            dp = split(dp_s[kc, at])
            z = z + jnp.sum(e, axis=0)
            s1 = s1 + jnp.sum(est, axis=0)
            d1 = d1 + jnp.sum(e * dp, axis=0)
            x1 = x1 + jnp.sum(est * dp, axis=0)
            y1 = y1 + jnp.sum(e * split(dpt_s[kc, at]), axis=0)
        for j, v in enumerate((m_new, z, s1, d1, x1, y1)):
            stats[t, j] = v

    def finish(t):
        m8, z, s1, d1, x1, y1 = [stats[t, j] for j in range(6)]
        top = jnp.max(m8, axis=0, keepdims=True)
        w8 = jnp.exp2(m8 - top)

        def total(v):
            return jnp.sum(v * w8, axis=0, keepdims=True)

        rz = 1.0 / total(z)
        tan_mean = total(s1) * rz
        delta = total(d1) * rz
        delta_tan = scaling * (total(x1) * rz - tan_mean * delta) + total(y1) * rz
        for j, v in enumerate((top, rz, tan_mean, delta, delta_tan)):
            stats[t, j] = jnp.broadcast_to(v, (8, ROWS))

    def grad_values(t, kc):
        s_s, st_s, dp_s, dpt_s = scores[t]
        top, rz, tan_mean, delta, delta_tan = [stats[t, j] for j in range(5)]
        f = jnp.exp2(mcs[t][kc] - top) * rz
        fc = f * scaling
        for k in range(0, CHUNK, piece):
            at = slice(k, k + piece)
            e = split(s_s[kc, at])
            p = e * f[None]
            pt = e * fc[None] * (split(st_s[kc, at]) - tan_mean[None])
            dd = split(dp_s[kc, at]) - delta[None]
            dst = pt * dd + p * (split(dpt_s[kc, at]) - delta_tan[None])
            for j, v in enumerate((dst, p * dd, pt)):
                xs[t][j, at] = v.reshape(piece, ROWS).astype(jnp.bfloat16)

    def grad_dots(i, group, kc):
        for t in group:
            x = xs[t][0:2].reshape(2 * CHUNK, ROWS)
            dqs[t][...] += dot(kts[kc], x, NN)
        left = jnp.concatenate([xs[t][j] for t in group for j in range(2)], axis=1)
        right = jnp.concatenate([qs[i, t, j] for t in group for j in range(2)], axis=0)
        dk = dot(left, right, NN)
        left = jnp.concatenate([xs[t][2] for t in group], axis=1)
        right = jnp.concatenate([qs[i, t, 2] for t in group], axis=0)
        dv = dot(left, right, NN)
        at = pl.ds(kc * per_chunk, per_chunk)
        acc[at, :, :HD] += dk.reshape(per_chunk, tokens, HD)
        acc[at, :, HD:] += dv.reshape(per_chunk, tokens, HD)

    def block(i, _):
        b = order_ref[jnp.where(i == 0, me, me ^ 1)]
        full = (b * tokens) // CHUNK
        stats[...] = jnp.zeros_like(stats)
        for t in range(tiles):
            stats[t, 0] = jnp.full((8, ROWS), FILL, jnp.float32)

        def score_step(kc, _, masked):
            score_dots(i, 0, kc, masked, b)
            for t in range(tiles):
                if t + 1 < tiles:
                    score_dots(i, t + 1, kc, masked, b)
                score_sums(t, kc)
            return 0

        lax.fori_loop(0, full, functools.partial(score_step, masked=False), 0)
        score_step(full, 0, True)
        for t in range(tiles):
            finish(t)
        for t in range(tiles):
            dqs[t][...] = jnp.zeros_like(dqs[t])

        def grad_step(kc, _):
            for at in range(0, tiles, span):
                for t in range(at, at + span):
                    grad_values(t, kc)
                if at:
                    grad_dots(i, range(at - span, at), kc)
            grad_dots(i, range(tiles - span, tiles), kc)
            return 0

        lax.fori_loop(0, full + 1, grad_step, 0)
        for t in range(tiles):
            dq = (dqs[t][...] * scaling).T.astype(jnp.bfloat16)
            wide = dq.astype(jnp.float32)
            sq_ref[...] += jnp.sum(split(wide * wide), axis=0)
            for h in range(per_tile):
                c = (t * per_tile + h) * HD
                dq_ref[i, :, c : c + HD] = dq[h * tokens : (h + 1) * tokens]
        return 0

    lax.fori_loop(0, 2, block, 0)

    for m, ref in enumerate(out_refs):
        for e in range(ref.shape[0] // tokens):
            block_at = acc[order_ref[out_seq(me, m, e)]]
            rows_at = slice(e * tokens, (e + 1) * tokens)
            ref[rows_at, :HD] = (block_at[:, :HD] * scaling).astype(ref.dtype)
            ref[rows_at, HD:] = block_at[:, HD:].astype(ref.dtype)


def run_hvp(me, order, q, qt, do, peer, own_kv, kvs, outs, seq_of, out_seq, col_of, width):
    tokens = q.shape[0]
    blocks = sum(k.shape[0] for k in kvs) + bool(own_kv)
    chunks = blocks * tokens // CHUNK
    tiles = width // ROWS
    f32 = jnp.float32
    score = pltpu.VMEM((chunks, CHUNK, ROWS), f32)
    kernel = functools.partial(
        hvp_kernel, seq_of, out_seq, len(own_kv), len(kvs), len(outs), tokens, width, col_of, HD ** (-0.5)
    )
    outs = [
        jax.ShapeDtypeStruct((2, tokens, width), jnp.bfloat16),
        jax.ShapeDtypeStruct((8, HD), f32),
    ] + outs
    flops = 2 * blocks * tokens * tokens * width * 10
    return pl.pallas_call(
        kernel,
        name="hvp",
        out_shape=outs,
        in_specs=[pl.BlockSpec(memory_space=pltpu.SMEM)]
        + [pl.BlockSpec(memory_space=pl.ANY)] * (5 + len(own_kv) + len(kvs)),
        out_specs=[pl.BlockSpec(memory_space=pltpu.VMEM)] * len(outs),
        scratch_shapes=[
            pltpu.VMEM((2, tiles, 3, ROWS, HD), jnp.bfloat16),
            pltpu.VMEM((blocks, tokens, 4 * HD), jnp.bfloat16),
            pltpu.VMEM((chunks, HD, 2 * CHUNK), jnp.bfloat16),
            pltpu.VMEM((blocks, tokens, 2 * HD), f32),
            pltpu.SemaphoreType.DMA((2,)),
            pltpu.VMEM((tiles, 6, 8, ROWS), f32),
            pltpu.SMEM(order.shape, jnp.int32),
        ]
        + [pltpu.VMEM((chunks, 8, ROWS), f32)] * tiles
        + [pltpu.VMEM((HD, ROWS), f32)] * tiles
        + [pltpu.VMEM((3, CHUNK, ROWS), jnp.bfloat16)] * tiles
        + [score] * (4 * tiles),
        compiler_params=pltpu.CompilerParams(vmem_limit_bytes=48 * 1024 * 1024),
        cost_estimate=pl.CostEstimate(flops=flops, bytes_accessed=4 << 20, transcendentals=0),
    )(me, order, q, qt, do, peer, *own_kv, *kvs)


def add_kernel(me_ref, own_ref, *rest):
    *got, dq_ref, dq_got_ref, sq_ref, dq_out, mine_ref, peer_ref, sum_ref, sem = rest
    width = dq_ref.shape[2]
    tokens = dq_ref.shape[1]
    core = lax.rem(me_ref[0], 2)
    mine = pl.multiple_of(core * width, HD)
    theirs = pl.multiple_of((1 - core) * width, HD)
    moves = (
        pltpu.make_async_copy(dq_ref.at[0], dq_out.at[:, pl.ds(mine, width)], sem.at[0]),
        pltpu.make_async_copy(dq_got_ref, dq_out.at[:, pl.ds(theirs, width)], sem.at[1]),
    )
    for move in moves:
        move.start()
    f32 = jnp.float32
    total = sq_ref[...]
    for e, out in enumerate((mine_ref, peer_ref)):
        rows = slice(e * tokens, (e + 1) * tokens)
        for cols in (slice(0, HD), slice(HD, 2 * HD)):
            final = own_ref[rows, cols]
            for ref in got:
                final = final + ref[rows, cols].astype(f32)
            final = final.astype(jnp.bfloat16)
            out[:, cols] = final
            wide = final.astype(f32)
            total = total + jnp.sum((wide * wide).reshape(-1, 8, HD), axis=0)
    line = jnp.sum(total, axis=0, keepdims=True)
    sum_ref[...] = jnp.broadcast_to(line[None], sum_ref.shape)
    for move in moves:
        move.wait()


def run_add(me, own, got, dq, dq_got, sq, devices):
    tokens, width = dq.shape[1:]
    half = jax.ShapeDtypeStruct((tokens, 2 * HD), jnp.bfloat16)
    return pl.pallas_call(
        add_kernel,
        name="add",
        out_shape=[
            jax.ShapeDtypeStruct((tokens, 2 * width), jnp.bfloat16),
            half,
            half,
            jax.ShapeDtypeStruct((devices, 1, HD), jnp.float32),
        ],
        in_specs=[pl.BlockSpec(memory_space=pltpu.SMEM)]
        + [pl.BlockSpec(memory_space=pltpu.VMEM)] * (len(got) + 4),
        out_specs=[pl.BlockSpec(memory_space=pl.ANY)]
        + [pl.BlockSpec(memory_space=pltpu.VMEM)] * 3,
        scratch_shapes=[pltpu.SemaphoreType.DMA((2,))],
        compiler_params=pltpu.CompilerParams(vmem_limit_bytes=4 << 20),
        cost_estimate=pl.CostEstimate(flops=1 << 20, bytes_accessed=2 << 20, transcendentals=0),
    )(me, own, *got, dq, dq_got, sq)


def pack_kernel(count, me_ref, *refs):
    core = lax.rem(me_ref[0], 2)
    sources, rows = refs[:count], refs[count:-4]
    theirs_ref, mine_ref, rows_ref, sem = refs[-4:]
    moves = []

    def move(ref, at, width, out, to):
        cols = pl.ds(pl.multiple_of(at * width, HD), width)
        moves.append(
            pltpu.make_async_copy(
                ref.at[:, cols], out.at[:, pl.ds(to * width, width)], sem.at[len(moves)]
            )
        )

    for out, head in ((theirs_ref, 1 - core), (mine_ref, core)):
        for j, ref in enumerate(sources):
            move(ref, head, HD, out, j)
    for j, ref in enumerate(rows):
        move(ref, 1 - core, ref.shape[1] // 2, rows_ref, j)
    for m in moves:
        m.start()
    for m in moves:
        m.wait()


def run_pack(me, sources, rows):
    tokens = rows[0].shape[0]
    half = jax.ShapeDtypeStruct((tokens, len(sources) * HD), sources[0].dtype)
    wide = jax.ShapeDtypeStruct((tokens, sum(r.shape[1] for r in rows) // 2), rows[0].dtype)
    count = 2 * len(sources) + len(rows)
    return pl.pallas_call(
        functools.partial(pack_kernel, len(sources)),
        name="pack",
        out_shape=[half, half, wide],
        in_specs=[pl.BlockSpec(memory_space=pltpu.SMEM)]
        + [pl.BlockSpec(memory_space=pltpu.HBM)] * (len(sources) + len(rows)),
        out_specs=[pl.BlockSpec(memory_space=pltpu.VMEM)] * 3,
        scratch_shapes=[pltpu.SemaphoreType.DMA((count,))],
        compiler_params=pltpu.CompilerParams(vmem_limit_bytes=60 * 1024 * 1024),
        cost_estimate=pl.CostEstimate(flops=1 << 16, bytes_accessed=1 << 21, transcendentals=0),
    )(me, *sources, *rows)


def last_kernel(me_ref, mine_ref, got_ref, lines_ref, dk_out, dv_out, norm_ref):
    core = lax.rem(me_ref[0], 2)
    for ref, at in ((mine_ref, core), (got_ref, 1 - core)):
        cols = pl.ds(pl.multiple_of(at * HD, HD), HD)
        dk_out[:, cols] = ref[:, :HD]
        dv_out[:, cols] = ref[:, HD:]
    norm_ref[0, 0] = jnp.sum(lines_ref[...])


def run_last(me, mine, got, lines):
    return pl.pallas_call(
        last_kernel,
        name="last",
        out_shape=[
            jax.ShapeDtypeStruct(mine.shape, mine.dtype),
            jax.ShapeDtypeStruct(mine.shape, mine.dtype),
            jax.ShapeDtypeStruct((1, 1), jnp.float32),
        ],
        in_specs=[pl.BlockSpec(memory_space=pltpu.SMEM)]
        + [pl.BlockSpec(memory_space=pltpu.VMEM)] * 3,
        out_specs=[pl.BlockSpec(memory_space=pltpu.VMEM)] * 2
        + [pl.BlockSpec(memory_space=pltpu.SMEM)],
        compiler_params=pltpu.CompilerParams(vmem_limit_bytes=4 << 20),
        cost_estimate=pl.CostEstimate(flops=1 << 16, bytes_accessed=1 << 18, transcendentals=0),
    )(me, mine, got, lines)


def shifted(x, axis, bit):
    size = lax.axis_size(axis)
    return lax.ppermute(x, axis, [(i, i ^ bit) for i in range(size)])


def all_sum(x, axes):
    for axis in axes:
        size = lax.axis_size(axis)
        if size & (size - 1):
            x = lax.psum(x, axis)
            continue
        bit = 1
        while bit < size:
            x = x + shifted(x, axis, bit)
            bit *= 2
    return x


def square_sum(x):
    w = x.astype(jnp.float32)
    return jnp.sum(w * w)


def join(core, mine, theirs):
    low = jnp.where(core == 0, mine, theirs)
    high = jnp.where(core == 0, theirs, mine)
    return jnp.concatenate([low, high], axis=1)


def body(queries, keys, values, q_tangent, k_tangent, v_tangent, out_grad, block_order):
    tokens = queries.shape[0]
    heads = keys.shape[1] // HD
    shards = lax.axis_size("seq")
    me = lax.axis_index("seq").astype(jnp.int32)
    core = lax.rem(me, 2)
    me_arr = me.reshape(1)
    width = heads * G * HD // 2
    other = (1 - core) * width
    f32 = jnp.float32

    def swap_rows(arrays):
        cut = [lax.dynamic_slice_in_dim(x, other, width, 1) for x in arrays]
        return shifted(jnp.concatenate(cut, axis=1), "seq", 1)

    rows = (queries, q_tangent, out_grad)

    def col_of(at):
        return lax.rem(at, 2) * width

    sources = (keys, k_tangent, values, v_tangent)


    if heads == 2 and shards == 8:
        theirs, mine, cut = run_pack(me_arr, sources, rows)
        peer_kv = shifted(theirs, "seq", 1)
        x_kv = [shifted(mine, "seq", 2), shifted(theirs, "seq", 3)]
        y_kv = [shifted(mine, "seq", 4), shifted(theirs, "seq", 5)]
        peer_rows = shifted(cut, "seq", 1)
        half = 2 * HD
        xy_a = shifted(jnp.stack([v[:, :half] for v in y_kv]), "seq", 2)
        xy_b = shifted(jnp.stack([v[:, half:] for v in x_kv]), "seq", 4)
        xy_kv = jnp.concatenate([xy_a, xy_b], axis=2)
        kvs = [v[None] for v in (peer_kv, *x_kv, *y_kv)] + [xy_kv]
        dq, sq, own, *parts = run_hvp(
            me_arr, block_order, *rows, peer_rows, sources, kvs,
            [jax.ShapeDtypeStruct((2 * tokens, 2 * HD), f32)]
            + [jax.ShapeDtypeStruct((2 * tokens, 2 * HD), jnp.bfloat16)] * (shards // 2 - 1),
            lambda at, m, e: at ^ (m + 1 + e), lambda at, m, e: at ^ (2 * m + e), col_of, width,
        )
        got = [shifted(p, "seq", 2 * m + 2) for m, p in enumerate(parts)]
        dq_got = shifted(dq[1], "seq", 1)
        devices = shards * lax.axis_size("head")
        dq_out, dkv_mine, dkv_peer, line = run_add(me_arr, own, got, dq, dq_got, sq, devices)
        dkv_got = shifted(dkv_peer, "seq", 1)
        lines = lax.all_to_all(line, ("head", "seq"), 0, 0)
        dk_out, dv_out, norm = run_last(me_arr, dkv_mine, dkv_got, lines)
        return (dq_out, dk_out, dv_out, norm[0, 0])
    assert heads == 1
    whole = lax.all_gather(jnp.concatenate(sources, axis=1), "seq", axis=0)
    dq, sq, parts = run_hvp(
        me_arr, block_order, *rows, swap_rows(rows), (), (whole,),
        [jax.ShapeDtypeStruct((shards * tokens, 2 * HD), jnp.bfloat16)],
        lambda at, m, e: e, lambda at, m, e: e, col_of, width,
    )
    final = lax.psum_scatter(parts, "seq", scatter_dimension=0, tiled=True)
    dq_out = join(core, dq[0], shifted(dq[1], "seq", 1))
    local = square_sum(final) + jnp.sum(sq)
    squared_norm = all_sum(local, ("seq", "head"))
    return (dq_out, final[:, :HD], final[:, HD:], squared_norm)


def solution(mesh):
    placed = (P("seq", "head"),) * 7 + (P(),)
    return jax.shard_map(
        body,
        mesh=mesh,
        in_specs=placed,
        out_specs=(P("seq", "head"), P("seq", "head"), P("seq", "head"), P()),
        check_vma=False,
    )
```

```python
import functools

import jax
import jax.numpy as jnp
from jax import lax
from jax.experimental import pallas as pl
from jax.experimental.pallas import tpu as pltpu
from jax.sharding import PartitionSpec as P

HD = 128
G = 8
ROWS = 256
CHUNK = 256
LOG2E = 1.4426950408889634
FILL = -1e30

NT = (((1,), (1,)), ((), ()))
NN = (((1,), (0,)), ((), ()))


def dot(a, b, dims):
    return lax.dot_general(a, b, dims, preferred_element_type=jnp.float32)


def hvp_kernel(
    seq_of, out_seq, n_own, n_kv, n_out, tokens, width, col_of, scaling,
    me_ref, order_hbm, q_ref, qt_ref, do_ref, peer_ref, *rest
):
    own_kv, rest = rest[:n_own], rest[n_own:]
    kv_refs = rest[:n_kv]
    dq_ref, sq_ref = rest[n_kv : n_kv + 2]
    out_refs = rest[n_kv + 2 : n_kv + 2 + n_out]
    rest = rest[n_kv + 2 + n_out :]
    groups = width // HD
    tiles = width // ROWS
    qs, kvs, kts, acc, sem, order_ref = rest[:6]
    rest = rest[6:]
    dqs, xs, rest = rest[:tiles], rest[tiles : 2 * tiles], rest[2 * tiles :]
    held = 5 * tiles + 1
    sets = len(rest) // held
    rest = [rest[w * held : (w + 1) * held] for w in range(sets)] * (3 - sets)
    stats_sets = [r[0] for r in rest]
    mcs = [r[1 : 1 + tiles] for r in rest]
    scores = [[r[1 + tiles + 4 * t :][:4] for t in range(tiles)] for r in rest]
    per_tile = ROWS // tokens
    me = me_ref[0]
    first = col_of(me)

    table = pltpu.make_async_copy(order_hbm, order_ref, sem.at[1])
    table.start()
    copies = []
    for which, ref in enumerate((q_ref, qt_ref, do_ref)):
        for g in range(groups):
            copies.append(
                pltpu.make_async_copy(
                    ref.at[:, pl.ds(pl.multiple_of(first + g * HD, HD), HD)],
                    qs.at[0, g // per_tile, which, pl.ds((g % per_tile) * tokens, tokens), :],
                    sem.at[0],
                )
            )
            copies.append(
                pltpu.make_async_copy(
                    peer_ref.at[:, pl.ds(which * width + g * HD, HD)],
                    qs.at[1, g // per_tile, which, pl.ds((g % per_tile) * tokens, tokens), :],
                    sem.at[0],
                )
            )
    for c in copies:
        c.start()
    table.wait()
    late = []
    for j, ref in enumerate(own_kv):
        head = pl.ds(pl.multiple_of(lax.rem(me, 2) * HD, HD), HD)
        to = kvs.at[order_ref[me], :, pl.ds(j * HD, HD)]
        late.append(pltpu.make_async_copy(ref.at[:, head], to, sem.at[0]))
    for m, ref in enumerate(kv_refs):
        for e in range(ref.shape[0]):
            at = order_ref[seq_of(me, m, e)]
            late.append(pltpu.make_async_copy(ref.at[e], kvs.at[at], sem.at[0]))
    for c in late:
        c.start()
    copies += late
    acc[...] = jnp.zeros_like(acc)
    sq_ref[...] = jnp.zeros_like(sq_ref)
    for c in copies:
        c.wait()

    blocks = kvs.shape[0]
    per_chunk = CHUNK // tokens
    chunks = blocks // per_chunk

    def chunk_kv(kc):
        return kvs[pl.ds(kc * per_chunk, per_chunk)].reshape(CHUNK, 4 * HD)

    def transpose_keys(kc, _):
        kv = chunk_kv(kc)
        kts[kc] = jnp.concatenate([kv[:, :HD].T, kv[:, HD : 2 * HD].T], axis=1)
        return 0

    lax.fori_loop(0, chunks, transpose_keys, 0)

    scale2 = scaling * LOG2E
    key_iota = lax.broadcasted_iota(jnp.int32, (CHUNK, ROWS), 0)
    row_iota = lax.rem(lax.broadcasted_iota(jnp.int32, (CHUNK, ROWS), 1), tokens)
    behind = row_iota - key_iota

    def split(x):
        return x.reshape(x.shape[0] // 8, 8, x.shape[1])

    piece = 32
    span = min(1, tiles)

    def score_dots(w, i, t, kc, masked, b):
        s_s, st_s, dp_s, dpt_s = scores[w][t]
        q, qt, do = qs[i, t, 0], qs[i, t, 1], qs[i, t, 2]
        kv = chunk_kv(kc)
        s = dot(kv[:, :HD], q, NT)
        if masked:
            s = jnp.where(behind >= kc * CHUNK - b * tokens, s, FILL)
        s_s[kc] = s
        st_s[kc] = dot(kv[:, : 2 * HD], jnp.concatenate([qt, q], axis=1), NT)
        both = dot(
            jnp.concatenate([kv[:, 2 * HD : 3 * HD], kv[:, 3 * HD :]], axis=0), do, NT
        )
        dp_s[kc] = both[:CHUNK]
        dpt_s[kc] = both[CHUNK:]

    def score_sums(w, t, kc):
        s_s, st_s, dp_s, dpt_s = scores[w][t]
        stats = stats_sets[w]
        m_old, z, s1, d1, x1, y1 = [stats[t, j] for j in range(6)]
        m_new = m_old
        for k in range(0, CHUNK, piece):
            s = split(s_s[kc, k : k + piece])
            m_new = jnp.maximum(m_new, jnp.max(s, axis=0) * scale2)
        decay = jnp.exp2(m_old - m_new)
        mcs[w][t][kc] = m_new
        z, s1, d1, x1, y1 = [v * decay for v in (z, s1, d1, x1, y1)]
        for k in range(0, CHUNK, piece):
            at = slice(k, k + piece)
            e = jnp.exp2(split(s_s[kc, at]) * scale2 - m_new[None])
            s_s[kc, at] = e.reshape(piece, ROWS)
            est = e * split(st_s[kc, at])
            dp = split(dp_s[kc, at])
            z = z + jnp.sum(e, axis=0)
            s1 = s1 + jnp.sum(est, axis=0)
            d1 = d1 + jnp.sum(e * dp, axis=0)
            x1 = x1 + jnp.sum(est * dp, axis=0)
            y1 = y1 + jnp.sum(e * split(dpt_s[kc, at]), axis=0)
        for j, v in enumerate((m_new, z, s1, d1, x1, y1)):
            stats[t, j] = v

    def finish(w, t):
        stats = stats_sets[w]
        m8, z, s1, d1, x1, y1 = [stats[t, j] for j in range(6)]
        top = jnp.max(m8, axis=0, keepdims=True)
        w8 = jnp.exp2(m8 - top)

        def total(v):
            return jnp.sum(v * w8, axis=0, keepdims=True)

        rz = 1.0 / total(z)
        tan_mean = total(s1) * rz
        delta = total(d1) * rz
        delta_tan = scaling * (total(x1) * rz - tan_mean * delta) + total(y1) * rz
        for j, v in enumerate((top, rz, tan_mean, delta, delta_tan)):
            stats[t, j] = jnp.broadcast_to(v, (8, ROWS))

    def grad_values(w, t, kc):
        s_s, st_s, dp_s, dpt_s = scores[w][t]
        stats = stats_sets[w]
        top, rz, tan_mean, delta, delta_tan = [stats[t, j] for j in range(5)]
        f = jnp.exp2(mcs[w][t][kc] - top) * rz
        fc = f * scaling
        for k in range(0, CHUNK, piece):
            at = slice(k, k + piece)
            e = split(s_s[kc, at])
            p = e * f[None]
            pt = e * fc[None] * (split(st_s[kc, at]) - tan_mean[None])
            dd = split(dp_s[kc, at]) - delta[None]
            dst = pt * dd + p * (split(dpt_s[kc, at]) - delta_tan[None])
            for j, v in enumerate((dst, p * dd, pt)):
                xs[t][j, at] = v.reshape(piece, ROWS).astype(jnp.bfloat16)

    def grad_dots(i, group, kc):
        for t in group:
            x = xs[t][0:2].reshape(2 * CHUNK, ROWS)
            dqs[t][...] += dot(kts[kc], x, NN)
        left = jnp.concatenate([xs[t][j] for t in group for j in range(2)], axis=1)
        right = jnp.concatenate([qs[i, t, j] for t in group for j in range(2)], axis=0)
        dk = dot(left, right, NN)
        left = jnp.concatenate([xs[t][2] for t in group], axis=1)
        right = jnp.concatenate([qs[i, t, 2] for t in group], axis=0)
        dv = dot(left, right, NN)
        at = pl.ds(kc * per_chunk, per_chunk)
        acc[at, :, :HD] += dk.reshape(per_chunk, tokens, HD)
        acc[at, :, HD:] += dv.reshape(per_chunk, tokens, HD)

    def score_step(kc, _, w, i, b, masked):
        score_dots(w, i, 0, kc, masked, b)
        for t in range(tiles):
            if t + 1 < tiles:
                score_dots(w, i, t + 1, kc, masked, b)
            score_sums(w, t, kc)
        return 0

    def grad_step(kc, _, w, i):
        for t in range(tiles):
            grad_values(w, t, kc)
            grad_dots(i, (t,), kc)
        return 0

    def both_step(kc, _):
        for t in range(tiles):
            score_dots(1, i1, t, kc, False, b1)
            grad_values(0, t, kc)
            grad_dots(i0, (t,), kc)
            score_sums(1, t, kc)
        return 0

    def clear(w):
        stats_sets[w][...] = jnp.zeros_like(stats_sets[w])
        for t in range(tiles):
            stats_sets[w][t, 0] = jnp.full((8, ROWS), FILL, jnp.float32)

    def clear_dq():
        for t in range(tiles):
            dqs[t][...] = jnp.zeros_like(dqs[t])

    def store_dq(i):
        for t in range(tiles):
            dq = (dqs[t][...] * scaling).T.astype(jnp.bfloat16)
            wide = dq.astype(jnp.float32)
            sq_ref[...] += jnp.sum(split(wide * wide), axis=0)
            for h in range(per_tile):
                c = (t * per_tile + h) * HD
                dq_ref[i, :, c : c + HD] = dq[h * tokens : (h + 1) * tokens]

    def run(low, high, step, **fixed):
        lax.fori_loop(low, high, functools.partial(step, **fixed), 0)

    own, peer = order_ref[me], order_ref[me ^ 1]
    i0 = (own > peer).astype(jnp.int32)
    i1 = 1 - i0
    b0, b1 = jnp.minimum(own, peer), jnp.maximum(own, peer)
    full0, full1 = (b0 * tokens) // CHUNK, (b1 * tokens) // CHUNK
    clear(0)
    run(0, full0, score_step, w=0, i=i0, b=b0, masked=False)
    score_step(full0, 0, 0, i0, b0, True)
    for t in range(tiles):
        finish(0, t)
    clear_dq()
    joint = 0
    if sets > 1:
        clear(1)
        joint = jnp.minimum(full0 + 1, full1)
        run(0, joint, both_step)
    run(joint, full0 + 1, grad_step, w=0, i=i0)
    store_dq(i0)
    clear_dq()
    if sets == 1:
        clear(1)
    run(joint, full1, score_step, w=1, i=i1, b=b1, masked=False)
    score_step(full1, 0, 1, i1, b1, True)
    for t in range(tiles):
        finish(1, t)
    run(0, full1 + 1, grad_step, w=1, i=i1)
    store_dq(i1)

    for m, ref in enumerate(out_refs):
        for e in range(ref.shape[0] // tokens):
            block_at = acc[order_ref[out_seq(me, m, e)]]
            rows_at = slice(e * tokens, (e + 1) * tokens)
            ref[rows_at, :HD] = (block_at[:, :HD] * scaling).astype(ref.dtype)
            ref[rows_at, HD:] = block_at[:, HD:].astype(ref.dtype)


def run_hvp(me, order, q, qt, do, peer, own_kv, kvs, outs, seq_of, out_seq, col_of, width):
    tokens = q.shape[0]
    blocks = sum(k.shape[0] for k in kvs) + bool(own_kv)
    chunks = blocks * tokens // CHUNK
    tiles = width // ROWS
    f32 = jnp.float32
    score = pltpu.VMEM((chunks, CHUNK, ROWS), f32)
    sets = 2 if 2 * 4 * tiles * chunks * CHUNK * ROWS * 4 <= 36 << 20 else 1
    kernel = functools.partial(
        hvp_kernel, seq_of, out_seq, len(own_kv), len(kvs), len(outs), tokens, width, col_of, HD ** (-0.5)
    )
    outs = [
        jax.ShapeDtypeStruct((2, tokens, width), jnp.bfloat16),
        jax.ShapeDtypeStruct((8, HD), f32),
    ] + outs
    flops = 2 * blocks * tokens * tokens * width * 10
    return pl.pallas_call(
        kernel,
        name="hvp",
        out_shape=outs,
        in_specs=[pl.BlockSpec(memory_space=pltpu.SMEM)]
        + [pl.BlockSpec(memory_space=pl.ANY)] * (5 + len(own_kv) + len(kvs)),
        out_specs=[pl.BlockSpec(memory_space=pltpu.VMEM)] * len(outs),
        scratch_shapes=[
            pltpu.VMEM((2, tiles, 3, ROWS, HD), jnp.bfloat16),
            pltpu.VMEM((blocks, tokens, 4 * HD), jnp.bfloat16),
            pltpu.VMEM((chunks, HD, 2 * CHUNK), jnp.bfloat16),
            pltpu.VMEM((blocks, tokens, 2 * HD), f32),
            pltpu.SemaphoreType.DMA((2,)),
            pltpu.SMEM(order.shape, jnp.int32),
        ]
        + [pltpu.VMEM((HD, ROWS), f32)] * tiles
        + [pltpu.VMEM((3, CHUNK, ROWS), jnp.bfloat16)] * tiles
        + sets
        * (
            [pltpu.VMEM((tiles, 6, 8, ROWS), f32)]
            + [pltpu.VMEM((chunks, 8, ROWS), f32)] * tiles
            + [score] * (4 * tiles)
        ),
        compiler_params=pltpu.CompilerParams(vmem_limit_bytes=48 * 1024 * 1024),
        cost_estimate=pl.CostEstimate(flops=flops, bytes_accessed=4 << 20, transcendentals=0),
    )(me, in_hbm(order), q, qt, do, peer, *own_kv, *kvs)


def add_kernel(me_ref, own_ref, *rest):
    *got, dq_ref, dq_got_ref, sq_ref, dq_out, mine_ref, peer_ref, sum_ref, sem = rest
    width = dq_ref.shape[2]
    tokens = dq_ref.shape[1]
    core = lax.rem(me_ref[0], 2)
    mine = pl.multiple_of(core * width, HD)
    theirs = pl.multiple_of((1 - core) * width, HD)
    moves = (
        pltpu.make_async_copy(dq_ref.at[0], dq_out.at[:, pl.ds(mine, width)], sem.at[0]),
        pltpu.make_async_copy(dq_got_ref, dq_out.at[:, pl.ds(theirs, width)], sem.at[1]),
    )
    for move in moves:
        move.start()
    f32 = jnp.float32
    total = sq_ref[...]
    for e, out in enumerate((mine_ref, peer_ref)):
        rows = slice(e * tokens, (e + 1) * tokens)
        for cols in (slice(0, HD), slice(HD, 2 * HD)):
            final = own_ref[rows, cols]
            for ref in got:
                final = final + ref[rows, cols].astype(f32)
            final = final.astype(jnp.bfloat16)
            out[:, cols] = final
            wide = final.astype(f32)
            total = total + jnp.sum((wide * wide).reshape(-1, 8, HD), axis=0)
    line = jnp.sum(total, axis=0, keepdims=True)
    sum_ref[...] = jnp.broadcast_to(line[None], sum_ref.shape)
    for move in moves:
        move.wait()


def run_add(me, own, got, dq, dq_got, sq, devices):
    tokens, width = dq.shape[1:]
    half = jax.ShapeDtypeStruct((tokens, 2 * HD), jnp.bfloat16)
    return pl.pallas_call(
        add_kernel,
        name="add",
        out_shape=[
            jax.ShapeDtypeStruct((tokens, 2 * width), jnp.bfloat16),
            half,
            half,
            jax.ShapeDtypeStruct((devices, 1, HD), jnp.float32),
        ],
        in_specs=[pl.BlockSpec(memory_space=pltpu.SMEM)]
        + [pl.BlockSpec(memory_space=pltpu.VMEM)] * (len(got) + 4),
        out_specs=[pl.BlockSpec(memory_space=pl.ANY)]
        + [pl.BlockSpec(memory_space=pltpu.VMEM)] * 3,
        scratch_shapes=[pltpu.SemaphoreType.DMA((2,))],
        compiler_params=pltpu.CompilerParams(vmem_limit_bytes=4 << 20),
        cost_estimate=pl.CostEstimate(flops=1 << 20, bytes_accessed=2 << 20, transcendentals=0),
    )(me, own, *got, dq, dq_got, sq)


def in_hbm(x):
    return pltpu.with_memory_space_constraint(x, pltpu.HBM)


def pack_kernel(count, me_ref, *refs):
    core = lax.rem(me_ref[0], 2)
    sources, rows = refs[:count], refs[count:-4]
    theirs_ref, mine_ref, rows_ref, sem = refs[-4:]
    moves = []

    def move(ref, at, width, out, to):
        cols = pl.ds(pl.multiple_of(at * width, HD), width)
        moves.append(
            pltpu.make_async_copy(
                ref.at[:, cols], out.at[:, pl.ds(to * width, width)], sem.at[len(moves)]
            )
        )

    for out, head in ((theirs_ref, 1 - core), (mine_ref, core)):
        for j, ref in enumerate(sources):
            move(ref, head, HD, out, j)
    for j, ref in enumerate(rows):
        move(ref, 1 - core, ref.shape[1] // 2, rows_ref, j)
    for m in moves:
        m.start()
    for m in moves:
        m.wait()


def run_pack(me, sources, rows):
    tokens = rows[0].shape[0]
    half = pltpu.VMEM((tokens, len(sources) * HD), sources[0].dtype)
    wide = pltpu.VMEM((tokens, sum(r.shape[1] for r in rows) // 2), rows[0].dtype)
    count = 2 * len(sources) + len(rows)
    return pl.pallas_call(
        functools.partial(pack_kernel, len(sources)),
        name="pack",
        out_shape=[half, half, wide],
        in_specs=[pl.BlockSpec(memory_space=pltpu.SMEM)]
        + [pl.BlockSpec(memory_space=pltpu.HBM)] * (len(sources) + len(rows)),
        out_specs=[pl.BlockSpec(memory_space=pltpu.VMEM)] * 3,
        scratch_shapes=[pltpu.SemaphoreType.DMA((count,))],
        compiler_params=pltpu.CompilerParams(vmem_limit_bytes=4 << 20),
        cost_estimate=pl.CostEstimate(flops=1 << 16, bytes_accessed=1 << 21, transcendentals=0),
    )(me, *map(in_hbm, sources), *map(in_hbm, rows))


def last_kernel(me_ref, mine_ref, got_ref, lines_ref, dk_out, dv_out, norm_ref):
    core = lax.rem(me_ref[0], 2)
    for ref, at in ((mine_ref, core), (got_ref, 1 - core)):
        cols = pl.ds(pl.multiple_of(at * HD, HD), HD)
        dk_out[:, cols] = ref[:, :HD]
        dv_out[:, cols] = ref[:, HD:]
    norm_ref[0, 0] = jnp.sum(lines_ref[...])


def run_last(me, mine, got, lines):
    return pl.pallas_call(
        last_kernel,
        name="last",
        out_shape=[
            jax.ShapeDtypeStruct(mine.shape, mine.dtype),
            jax.ShapeDtypeStruct(mine.shape, mine.dtype),
            jax.ShapeDtypeStruct((1, 1), jnp.float32),
        ],
        in_specs=[pl.BlockSpec(memory_space=pltpu.SMEM)]
        + [pl.BlockSpec(memory_space=pltpu.VMEM)] * 3,
        out_specs=[pl.BlockSpec(memory_space=pltpu.VMEM)] * 2
        + [pl.BlockSpec(memory_space=pltpu.SMEM)],
        compiler_params=pltpu.CompilerParams(vmem_limit_bytes=4 << 20),
        cost_estimate=pl.CostEstimate(flops=1 << 16, bytes_accessed=1 << 18, transcendentals=0),
    )(me, mine, got, lines)


def shifted(x, axis, bit):
    size = lax.axis_size(axis)
    return lax.ppermute(x, axis, [(i, i ^ bit) for i in range(size)])


def all_sum(x, axes):
    for axis in axes:
        size = lax.axis_size(axis)
        if size & (size - 1):
            x = lax.psum(x, axis)
            continue
        bit = 1
        while bit < size:
            x = x + shifted(x, axis, bit)
            bit *= 2
    return x


def square_sum(x):
    w = x.astype(jnp.float32)
    return jnp.sum(w * w)


def join(core, mine, theirs):
    low = jnp.where(core == 0, mine, theirs)
    high = jnp.where(core == 0, theirs, mine)
    return jnp.concatenate([low, high], axis=1)


def body(queries, keys, values, q_tangent, k_tangent, v_tangent, out_grad, block_order):
    tokens = queries.shape[0]
    heads = keys.shape[1] // HD
    shards = lax.axis_size("seq")
    me = lax.axis_index("seq").astype(jnp.int32)
    core = lax.rem(me, 2)
    me_arr = me.reshape(1)
    width = heads * G * HD // 2
    other = (1 - core) * width
    f32 = jnp.float32

    def swap_rows(arrays):
        cut = [lax.dynamic_slice_in_dim(x, other, width, 1) for x in arrays]
        return shifted(jnp.concatenate(cut, axis=1), "seq", 1)

    rows = (queries, q_tangent, out_grad)

    def col_of(at):
        return lax.rem(at, 2) * width

    sources = (keys, k_tangent, values, v_tangent)


    if heads == 2 and shards == 8:
        theirs, mine, cut = run_pack(me_arr, sources, rows)
        peer_kv = shifted(theirs, "seq", 1)
        x_kv = [shifted(mine, "seq", 2), shifted(theirs, "seq", 3)]
        y_kv = [shifted(mine, "seq", 4), shifted(theirs, "seq", 5)]
        peer_rows = shifted(cut, "seq", 1)
        half = 2 * HD
        xy_a = shifted(jnp.stack([v[:, :half] for v in y_kv]), "seq", 2)
        xy_b = shifted(jnp.stack([v[:, half:] for v in x_kv]), "seq", 4)
        xy_kv = jnp.concatenate([xy_a, xy_b], axis=2)
        kvs = [v[None] for v in (peer_kv, *x_kv, *y_kv)] + [xy_kv]
        dq, sq, own, *parts = run_hvp(
            me_arr, block_order, *rows, peer_rows, sources, kvs,
            [jax.ShapeDtypeStruct((2 * tokens, 2 * HD), f32)]
            + [jax.ShapeDtypeStruct((2 * tokens, 2 * HD), jnp.bfloat16)] * (shards // 2 - 1),
            lambda at, m, e: at ^ (m + 1 + e), lambda at, m, e: at ^ (2 * m + e), col_of, width,
        )
        got = [shifted(p, "seq", 2 * m + 2) for m, p in enumerate(parts)]
        dq_got = shifted(dq[1], "seq", 1)
        devices = shards * lax.axis_size("head")
        dq_out, dkv_mine, dkv_peer, line = run_add(me_arr, own, got, dq, dq_got, sq, devices)
        dkv_got = shifted(dkv_peer, "seq", 1)
        lines = lax.all_to_all(line, ("head", "seq"), 0, 0)
        dk_out, dv_out, norm = run_last(me_arr, dkv_mine, dkv_got, lines)
        return (dq_out, dk_out, dv_out, norm[0, 0])
    assert heads == 1
    whole = lax.all_gather(jnp.concatenate(sources, axis=1), "seq", axis=0)
    dq, sq, parts = run_hvp(
        me_arr, block_order, *rows, swap_rows(rows), (), (whole,),
        [jax.ShapeDtypeStruct((shards * tokens, 2 * HD), jnp.bfloat16)],
        lambda at, m, e: e, lambda at, m, e: e, col_of, width,
    )
    final = lax.psum_scatter(parts, "seq", scatter_dimension=0, tiled=True)
    dq_out = join(core, dq[0], shifted(dq[1], "seq", 1))
    local = square_sum(final) + jnp.sum(sq)
    squared_norm = all_sum(local, ("seq", "head"))
    return (dq_out, final[:, :HD], final[:, HD:], squared_norm)


def solution(mesh):
    placed = (P("seq", "head"),) * 7 + (P(),)
    return jax.shard_map(
        body,
        mesh=mesh,
        in_specs=placed,
        out_specs=(P("seq", "head"), P("seq", "head"), P("seq", "head"), P()),
        check_vma=False,
    )
```

```python
import functools

import jax
import jax.numpy as jnp
from jax import lax
from jax.experimental import pallas as pl
from jax.experimental.pallas import tpu as pltpu
from jax.sharding import PartitionSpec as P

HD = 128
G = 8
ROWS = 256
CHUNK = 256
LOG2E = 1.4426950408889634
FILL = -1e30

NT = (((1,), (1,)), ((), ()))
NN = (((1,), (0,)), ((), ()))


def dot(a, b, dims):
    return lax.dot_general(a, b, dims, preferred_element_type=jnp.float32)


def hvp_kernel(
    seq_of, out_seq, n_kv, n_out, tokens, width, col_of, scaling,
    me_ref, order_any, q_ref, qt_ref, do_ref, peer_ref, *rest
):
    kv_refs = rest[:n_kv]
    dq_ref, sq_ref = rest[n_kv : n_kv + 2]
    out_refs = rest[n_kv + 2 : n_kv + 2 + n_out]
    rest = rest[n_kv + 2 + n_out :]
    groups = width // HD
    tiles = width // ROWS
    qs, kvs, kts, acc, sem, order_ref = rest[:6]
    rest = rest[6:]
    dqs, xs, rest = rest[:tiles], rest[tiles : 2 * tiles], rest[2 * tiles :]
    held = 5 * tiles + 1
    sets = len(rest) // held
    rest = [rest[w * held : (w + 1) * held] for w in range(sets)] * (3 - sets)
    stats_sets = [r[0] for r in rest]
    mcs = [r[1 : 1 + tiles] for r in rest]
    scores = [[r[1 + tiles + 4 * t :][:4] for t in range(tiles)] for r in rest]
    per_tile = ROWS // tokens
    me = me_ref[0]
    first = col_of(me)

    table = pltpu.make_async_copy(order_any, order_ref, sem.at[1])
    table.start()
    copies = []
    for which, ref in enumerate((q_ref, qt_ref, do_ref)):
        for g in range(groups):
            copies.append(
                pltpu.make_async_copy(
                    ref.at[:, pl.ds(pl.multiple_of(first + g * HD, HD), HD)],
                    qs.at[0, g // per_tile, which, pl.ds((g % per_tile) * tokens, tokens), :],
                    sem.at[0],
                )
            )
            copies.append(
                pltpu.make_async_copy(
                    peer_ref.at[:, pl.ds(which * width + g * HD, HD)],
                    qs.at[1, g // per_tile, which, pl.ds((g % per_tile) * tokens, tokens), :],
                    sem.at[0],
                )
            )
    for c in copies:
        c.start()
    acc[...] = jnp.zeros_like(acc)
    sq_ref[...] = jnp.zeros_like(sq_ref)
    table.wait()
    late = []
    for m, ref in enumerate(kv_refs):
        for e in range(ref.shape[0]):
            at = order_ref[seq_of(me, m, e)]
            late.append(pltpu.make_async_copy(ref.at[e], kvs.at[at], sem.at[0]))
    for c in late:
        c.start()
    copies += late
    for c in copies:
        c.wait()

    blocks = kvs.shape[0]
    per_chunk = CHUNK // tokens
    chunks = blocks // per_chunk

    def chunk_kv(kc):
        return kvs[pl.ds(kc * per_chunk, per_chunk)].reshape(CHUNK, 4 * HD)

    def transpose_keys(kc):
        kv = chunk_kv(kc)
        kts[kc, :, :CHUNK] = kv[:, :HD].T
        kts[kc, :, CHUNK:] = kv[:, HD : 2 * HD].T

    scale2 = scaling * LOG2E
    key_iota = lax.broadcasted_iota(jnp.int32, (CHUNK, ROWS), 0)
    row_iota = lax.rem(lax.broadcasted_iota(jnp.int32, (CHUNK, ROWS), 1), tokens)
    behind = row_iota - key_iota

    def split(x):
        return x.reshape(x.shape[0] // 8, 8, x.shape[1])

    piece = 32
    span = min(1, tiles)

    def score_dots(w, i, t, kc, masked, b):
        s_s, st_s, dp_s, dpt_s = scores[w][t]
        q, qt, do = qs[i, t, 0], qs[i, t, 1], qs[i, t, 2]
        kv = chunk_kv(kc)
        s = dot(kv[:, :HD], q, NT)
        if masked:
            s = jnp.where(behind >= kc * CHUNK - b * tokens, s, FILL)
        s_s[kc] = s
        st_s[kc] = dot(kv[:, : 2 * HD], jnp.concatenate([qt, q], axis=1), NT)
        both = dot(
            jnp.concatenate([kv[:, 2 * HD : 3 * HD], kv[:, 3 * HD :]], axis=0), do, NT
        )
        dp_s[kc] = both[:CHUNK]
        dpt_s[kc] = both[CHUNK:]

    def score_sums(w, t, kc):
        s_s, st_s, dp_s, dpt_s = scores[w][t]
        stats = stats_sets[w]
        m_old, z, s1, d1, x1, y1 = [stats[t, j] for j in range(6)]
        m_new = m_old
        for k in range(0, CHUNK, piece):
            s = split(s_s[kc, k : k + piece])
            m_new = jnp.maximum(m_new, jnp.max(s, axis=0) * scale2)
        decay = jnp.exp2(m_old - m_new)
        mcs[w][t][kc] = m_new
        z, s1, d1, x1, y1 = [v * decay for v in (z, s1, d1, x1, y1)]
        for k in range(0, CHUNK, piece):
            at = slice(k, k + piece)
            e = jnp.exp2(split(s_s[kc, at]) * scale2 - m_new[None])
            s_s[kc, at] = e.reshape(piece, ROWS)
            est = e * split(st_s[kc, at])
            dp = split(dp_s[kc, at])
            z = z + jnp.sum(e, axis=0)
            s1 = s1 + jnp.sum(est, axis=0)
            d1 = d1 + jnp.sum(e * dp, axis=0)
            x1 = x1 + jnp.sum(est * dp, axis=0)
            y1 = y1 + jnp.sum(e * split(dpt_s[kc, at]), axis=0)
        for j, v in enumerate((m_new, z, s1, d1, x1, y1)):
            stats[t, j] = v

    def finish(w, t):
        stats = stats_sets[w]
        m8, z, s1, d1, x1, y1 = [stats[t, j] for j in range(6)]
        top = jnp.max(m8, axis=0, keepdims=True)
        w8 = jnp.exp2(m8 - top)

        def total(v):
            return jnp.sum(v * w8, axis=0, keepdims=True)

        rz = 1.0 / total(z)
        tan_mean = total(s1) * rz
        delta = total(d1) * rz
        delta_tan = scaling * (total(x1) * rz - tan_mean * delta) + total(y1) * rz
        for j, v in enumerate((top, rz, tan_mean, delta, delta_tan)):
            stats[t, j] = jnp.broadcast_to(v, (8, ROWS))

    def grad_values(w, t, kc):
        s_s, st_s, dp_s, dpt_s = scores[w][t]
        stats = stats_sets[w]
        top, rz, tan_mean, delta, delta_tan = [stats[t, j] for j in range(5)]
        f = jnp.exp2(mcs[w][t][kc] - top) * rz
        fc = f * scaling
        for k in range(0, CHUNK, piece):
            at = slice(k, k + piece)
            e = split(s_s[kc, at])
            p = e * f[None]
            pt = e * fc[None] * (split(st_s[kc, at]) - tan_mean[None])
            dd = split(dp_s[kc, at]) - delta[None]
            dst = pt * dd + p * (split(dpt_s[kc, at]) - delta_tan[None])
            for j, v in enumerate((dst, p * dd, pt)):
                xs[t][j, at] = v.reshape(piece, ROWS).astype(jnp.bfloat16)

    def grad_dots(i, group, kc):
        for t in group:
            x = xs[t][0:2].reshape(2 * CHUNK, ROWS)
            dqs[t][...] += dot(kts[kc], x, NN)
        left = jnp.concatenate([xs[t][j] for t in group for j in range(2)], axis=1)
        right = jnp.concatenate([qs[i, t, j] for t in group for j in range(2)], axis=0)
        dk = dot(left, right, NN)
        left = jnp.concatenate([xs[t][2] for t in group], axis=1)
        right = jnp.concatenate([qs[i, t, 2] for t in group], axis=0)
        dv = dot(left, right, NN)
        at = pl.ds(kc * per_chunk, per_chunk)
        acc[at, :, :HD] += dk.reshape(per_chunk, tokens, HD)
        acc[at, :, HD:] += dv.reshape(per_chunk, tokens, HD)

    def score_step(kc, _, w, i, b, masked):
        score_dots(w, i, 0, kc, masked, b)
        transpose_keys(kc)
        for t in range(tiles):
            if t + 1 < tiles:
                score_dots(w, i, t + 1, kc, masked, b)
            score_sums(w, t, kc)
        return 0

    def grad_step(kc, _, w, i):
        for t in range(tiles):
            grad_values(w, t, kc)
            grad_dots(i, (t,), kc)
        return 0

    def both_step(kc, _):
        for t in range(tiles):
            score_dots(1, i1, t, kc, False, b1)
            grad_values(0, t, kc)
            grad_dots(i0, (t,), kc)
            score_sums(1, t, kc)
        return 0

    def clear(w):
        stats_sets[w][...] = jnp.zeros_like(stats_sets[w])
        for t in range(tiles):
            stats_sets[w][t, 0] = jnp.full((8, ROWS), FILL, jnp.float32)

    def clear_dq():
        for t in range(tiles):
            dqs[t][...] = jnp.zeros_like(dqs[t])

    def store_dq(i):
        for t in range(tiles):
            dq = (dqs[t][...] * scaling).T.astype(jnp.bfloat16)
            wide = dq.astype(jnp.float32)
            sq_ref[...] += jnp.sum(split(wide * wide), axis=0)
            for h in range(per_tile):
                c = (t * per_tile + h) * HD
                dq_ref[i, :, c : c + HD] = dq[h * tokens : (h + 1) * tokens]

    def run(low, high, step, **fixed):
        lax.fori_loop(low, high, functools.partial(step, **fixed), 0)

    own, peer = order_ref[me], order_ref[me ^ 1]
    i0 = (own > peer).astype(jnp.int32)
    i1 = 1 - i0
    b0, b1 = jnp.minimum(own, peer), jnp.maximum(own, peer)
    full0, full1 = (b0 * tokens) // CHUNK, (b1 * tokens) // CHUNK
    clear(0)
    run(0, full0, score_step, w=0, i=i0, b=b0, masked=False)
    score_step(full0, 0, 0, i0, b0, True)
    for t in range(tiles):
        finish(0, t)
    clear_dq()
    joint = 0
    if sets > 1:
        clear(1)
        joint = jnp.minimum(full0 + 1, full1)
        run(0, joint, both_step)
    run(joint, full0 + 1, grad_step, w=0, i=i0)
    store_dq(i0)
    clear_dq()
    if sets == 1:
        clear(1)
    run(joint, full1, score_step, w=1, i=i1, b=b1, masked=False)
    score_step(full1, 0, 1, i1, b1, True)
    for t in range(tiles):
        finish(1, t)
    run(0, full1 + 1, grad_step, w=1, i=i1)
    store_dq(i1)

    for m, ref in enumerate(out_refs):
        for e in range(ref.shape[0] // tokens):
            block_at = acc[order_ref[out_seq(me, m, e)]]
            rows_at = slice(e * tokens, (e + 1) * tokens)
            ref[rows_at, :HD] = (block_at[:, :HD] * scaling).astype(ref.dtype)
            ref[rows_at, HD:] = block_at[:, HD:].astype(ref.dtype)


def run_hvp(me, order, q, qt, do, peer, kvs, outs, seq_of, out_seq, col_of, width):
    tokens = q.shape[0]
    blocks = sum(k.shape[0] for k in kvs)
    chunks = blocks * tokens // CHUNK
    tiles = width // ROWS
    f32 = jnp.float32
    score = pltpu.VMEM((chunks, CHUNK, ROWS), f32)
    sets = 2 if 2 * 4 * tiles * chunks * CHUNK * ROWS * 4 <= 36 << 20 else 1
    kernel = functools.partial(
        hvp_kernel, seq_of, out_seq, len(kvs), len(outs), tokens, width, col_of, HD ** (-0.5)
    )
    outs = [
        jax.ShapeDtypeStruct((2, tokens, width), jnp.bfloat16),
        jax.ShapeDtypeStruct((8, HD), f32),
    ] + outs
    flops = 2 * blocks * tokens * tokens * width * 10
    return pl.pallas_call(
        kernel,
        name="hvp",
        out_shape=outs,
        in_specs=[pl.BlockSpec(memory_space=pltpu.SMEM)]
        + [pl.BlockSpec(memory_space=pl.ANY)] * (5 + len(kvs)),
        out_specs=[pl.BlockSpec(memory_space=pltpu.VMEM)] * len(outs),
        scratch_shapes=[
            pltpu.VMEM((2, tiles, 3, ROWS, HD), jnp.bfloat16),
            pltpu.VMEM((blocks, tokens, 4 * HD), jnp.bfloat16),
            pltpu.VMEM((chunks, HD, 2 * CHUNK), jnp.bfloat16),
            pltpu.VMEM((blocks, tokens, 2 * HD), f32),
            pltpu.SemaphoreType.DMA((2,)),
            pltpu.SMEM(order.shape, jnp.int32),
        ]
        + [pltpu.VMEM((HD, ROWS), f32)] * tiles
        + [pltpu.VMEM((3, CHUNK, ROWS), jnp.bfloat16)] * tiles
        + sets
        * (
            [pltpu.VMEM((tiles, 6, 8, ROWS), f32)]
            + [pltpu.VMEM((chunks, 8, ROWS), f32)] * tiles
            + [score] * (4 * tiles)
        ),
        compiler_params=pltpu.CompilerParams(vmem_limit_bytes=48 * 1024 * 1024),
        cost_estimate=pl.CostEstimate(flops=flops, bytes_accessed=4 << 20, transcendentals=0),
    )(me, order, q, qt, do, peer, *kvs)


def add_kernel(me_ref, own_ref, *rest):
    *got, dq_ref, dq_got_ref, sq_ref, dq_out, mine_ref, peer_ref, sum_ref, sem = rest
    width = dq_ref.shape[2]
    tokens = dq_ref.shape[1]
    core = lax.rem(me_ref[0], 2)
    mine = pl.multiple_of(core * width, HD)
    theirs = pl.multiple_of((1 - core) * width, HD)
    moves = (
        pltpu.make_async_copy(dq_ref.at[0], dq_out.at[:, pl.ds(mine, width)], sem.at[0]),
        pltpu.make_async_copy(dq_got_ref, dq_out.at[:, pl.ds(theirs, width)], sem.at[1]),
    )
    for move in moves:
        move.start()
    f32 = jnp.float32
    total = sq_ref[...]
    for e, out in enumerate((mine_ref, peer_ref)):
        rows = slice(e * tokens, (e + 1) * tokens)
        for cols in (slice(0, HD), slice(HD, 2 * HD)):
            final = own_ref[rows, cols]
            for ref in got:
                final = final + ref[rows, cols].astype(f32)
            final = final.astype(jnp.bfloat16)
            out[:, cols] = final
            wide = final.astype(f32)
            total = total + jnp.sum((wide * wide).reshape(-1, 8, HD), axis=0)
    line = jnp.sum(total, axis=0, keepdims=True)
    sum_ref[...] = jnp.broadcast_to(line[None], sum_ref.shape)
    for move in moves:
        move.wait()


def run_add(me, own, got, dq, dq_got, sq, devices):
    tokens, width = dq.shape[1:]
    half = jax.ShapeDtypeStruct((tokens, 2 * HD), jnp.bfloat16)
    return pl.pallas_call(
        add_kernel,
        name="add",
        out_shape=[
            jax.ShapeDtypeStruct((tokens, 2 * width), jnp.bfloat16),
            half,
            half,
            jax.ShapeDtypeStruct((devices, 1, HD), jnp.float32),
        ],
        in_specs=[pl.BlockSpec(memory_space=pltpu.SMEM)]
        + [pl.BlockSpec(memory_space=pltpu.VMEM)] * (len(got) + 4),
        out_specs=[pl.BlockSpec(memory_space=pl.ANY)]
        + [pl.BlockSpec(memory_space=pltpu.VMEM)] * 3,
        scratch_shapes=[pltpu.SemaphoreType.DMA((2,))],
        compiler_params=pltpu.CompilerParams(vmem_limit_bytes=4 << 20),
        cost_estimate=pl.CostEstimate(flops=1 << 20, bytes_accessed=2 << 20, transcendentals=0),
    )(me, own, *got, dq, dq_got, sq)


def in_hbm(x):
    return pltpu.with_memory_space_constraint(x, pltpu.HBM)


def pack_kernel(count, me_ref, order_ref, *refs):
    core = lax.rem(me_ref[0], 2)
    sources, rows = refs[:count], refs[count:-5]
    theirs_ref, mine_ref, rows_ref, table_ref, sem = refs[-5:]
    moves = [pltpu.make_async_copy(order_ref, table_ref, sem.at[0])]

    def move(ref, at, width, out, to):
        cols = pl.ds(pl.multiple_of(at * width, HD), width)
        moves.append(
            pltpu.make_async_copy(
                ref.at[:, cols], out.at[:, pl.ds(to * width, width)], sem.at[len(moves)]
            )
        )

    for out, head in ((theirs_ref, 1 - core), (mine_ref, core)):
        for j, ref in enumerate(sources):
            move(ref, head, HD, out, j)
    for j, ref in enumerate(rows):
        move(ref, 1 - core, ref.shape[1] // 2, rows_ref, j)
    for m in moves:
        m.start()
    for m in moves:
        m.wait()


def run_pack(me, order, sources, rows):
    tokens = rows[0].shape[0]
    half = pltpu.VMEM((tokens, len(sources) * HD), sources[0].dtype)
    wide = pltpu.VMEM((tokens, sum(r.shape[1] for r in rows) // 2), rows[0].dtype)
    count = 1 + 2 * len(sources) + len(rows)
    return pl.pallas_call(
        functools.partial(pack_kernel, len(sources)),
        name="pack",
        out_shape=[half, half, wide, pltpu.VMEM(order.shape, order.dtype)],
        in_specs=[pl.BlockSpec(memory_space=pltpu.SMEM)]
        + [pl.BlockSpec(memory_space=pltpu.HBM)] * (1 + len(sources) + len(rows)),
        out_specs=[pl.BlockSpec(memory_space=pltpu.VMEM)] * 4,
        scratch_shapes=[pltpu.SemaphoreType.DMA((count,))],
        compiler_params=pltpu.CompilerParams(vmem_limit_bytes=4 << 20),
        cost_estimate=pl.CostEstimate(flops=1 << 16, bytes_accessed=1 << 21, transcendentals=0),
    )(me, *map(in_hbm, (order, *sources, *rows)))


def last_kernel(me_ref, mine_ref, got_ref, lines_ref, dk_out, dv_out, norm_ref):
    core = lax.rem(me_ref[0], 2)
    for ref, at in ((mine_ref, core), (got_ref, 1 - core)):
        cols = pl.ds(pl.multiple_of(at * HD, HD), HD)
        dk_out[:, cols] = ref[:, :HD]
        dv_out[:, cols] = ref[:, HD:]
    norm_ref[0, 0] = jnp.sum(lines_ref[...])


def run_last(me, mine, got, lines):
    return pl.pallas_call(
        last_kernel,
        name="last",
        out_shape=[
            jax.ShapeDtypeStruct(mine.shape, mine.dtype),
            jax.ShapeDtypeStruct(mine.shape, mine.dtype),
            jax.ShapeDtypeStruct((1, 1), jnp.float32),
        ],
        in_specs=[pl.BlockSpec(memory_space=pltpu.SMEM)]
        + [pl.BlockSpec(memory_space=pltpu.VMEM)] * 3,
        out_specs=[pl.BlockSpec(memory_space=pltpu.VMEM)] * 2
        + [pl.BlockSpec(memory_space=pltpu.SMEM)],
        compiler_params=pltpu.CompilerParams(vmem_limit_bytes=4 << 20),
        cost_estimate=pl.CostEstimate(flops=1 << 16, bytes_accessed=1 << 18, transcendentals=0),
    )(me, mine, got, lines)


def shifted(x, axis, bit):
    size = lax.axis_size(axis)
    return lax.ppermute(x, axis, [(i, i ^ bit) for i in range(size)])


def all_sum(x, axes):
    for axis in axes:
        size = lax.axis_size(axis)
        if size & (size - 1):
            x = lax.psum(x, axis)
            continue
        bit = 1
        while bit < size:
            x = x + shifted(x, axis, bit)
            bit *= 2
    return x


def square_sum(x):
    w = x.astype(jnp.float32)
    return jnp.sum(w * w)


def join(core, mine, theirs):
    low = jnp.where(core == 0, mine, theirs)
    high = jnp.where(core == 0, theirs, mine)
    return jnp.concatenate([low, high], axis=1)


def body(queries, keys, values, q_tangent, k_tangent, v_tangent, out_grad, block_order):
    tokens = queries.shape[0]
    heads = keys.shape[1] // HD
    shards = lax.axis_size("seq")
    me = lax.axis_index("seq").astype(jnp.int32)
    core = lax.rem(me, 2)
    me_arr = me.reshape(1)
    width = heads * G * HD // 2
    other = (1 - core) * width
    f32 = jnp.float32

    def swap_rows(arrays):
        cut = [lax.dynamic_slice_in_dim(x, other, width, 1) for x in arrays]
        return shifted(jnp.concatenate(cut, axis=1), "seq", 1)

    rows = (queries, q_tangent, out_grad)

    def col_of(at):
        return lax.rem(at, 2) * width

    sources = (keys, k_tangent, values, v_tangent)


    if heads == 2 and shards == 8:
        theirs, mine, cut, table = run_pack(me_arr, block_order, sources, rows)
        peer_kv = shifted(theirs, "seq", 1)
        x_kv = [shifted(mine, "seq", 2), shifted(theirs, "seq", 3)]
        y_kv = [shifted(mine, "seq", 4), shifted(theirs, "seq", 5)]
        peer_rows = shifted(cut, "seq", 1)
        half = 2 * HD
        xy_a = shifted(jnp.stack([v[:, :half] for v in y_kv]), "seq", 2)
        xy_b = shifted(jnp.stack([v[:, half:] for v in x_kv]), "seq", 4)
        xy_kv = jnp.concatenate([xy_a, xy_b], axis=2)
        kvs = [v[None] for v in (mine, peer_kv, *x_kv, *y_kv)] + [xy_kv]
        dq, sq, own, *parts = run_hvp(
            me_arr, table, *rows, peer_rows, kvs,
            [jax.ShapeDtypeStruct((2 * tokens, 2 * HD), f32)]
            + [jax.ShapeDtypeStruct((2 * tokens, 2 * HD), jnp.bfloat16)] * (shards // 2 - 1),
            lambda at, m, e: at ^ (m + e), lambda at, m, e: at ^ (2 * m + e), col_of, width,
        )
        got = [shifted(p, "seq", 2 * m + 2) for m, p in enumerate(parts)]
        dq_got = shifted(dq[1], "seq", 1)
        devices = shards * lax.axis_size("head")
        dq_out, dkv_mine, dkv_peer, line = run_add(me_arr, own, got, dq, dq_got, sq, devices)
        dkv_got = shifted(dkv_peer, "seq", 1)
        lines = lax.all_to_all(line, ("head", "seq"), 0, 0)
        dk_out, dv_out, norm = run_last(me_arr, dkv_mine, dkv_got, lines)
        return (dq_out, dk_out, dv_out, norm[0, 0])
    assert heads == 1
    whole = lax.all_gather(jnp.concatenate(sources, axis=1), "seq", axis=0)
    dq, sq, parts = run_hvp(
        me_arr, block_order, *rows, swap_rows(rows), (whole,),
        [jax.ShapeDtypeStruct((shards * tokens, 2 * HD), jnp.bfloat16)],
        lambda at, m, e: e, lambda at, m, e: e, col_of, width,
    )
    final = lax.psum_scatter(parts, "seq", scatter_dimension=0, tiled=True)
    dq_out = join(core, dq[0], shifted(dq[1], "seq", 1))
    local = square_sum(final) + jnp.sum(sq)
    squared_norm = all_sum(local, ("seq", "head"))
    return (dq_out, final[:, :HD], final[:, HD:], squared_norm)


def solution(mesh):
    placed = (P("seq", "head"),) * 7 + (P(),)
    return jax.shard_map(
        body,
        mesh=mesh,
        in_specs=placed,
        out_specs=(P("seq", "head"), P("seq", "head"), P("seq", "head"), P()),
        check_vma=False,
    )
```

```python
import functools

import jax
import jax.numpy as jnp
from jax import lax
from jax.experimental import pallas as pl
from jax.experimental.pallas import tpu as pltpu
from jax.sharding import PartitionSpec as P

HD = 128
G = 8
ROWS = 256
CHUNK = 256
LOG2E = 1.4426950408889634
FILL = -1e30

NT = (((1,), (1,)), ((), ()))
NN = (((1,), (0,)), ((), ()))


def dot(a, b, dims):
    return lax.dot_general(a, b, dims, preferred_element_type=jnp.float32)


def hvp_kernel(
    seq_of, out_seq, n_kv, n_out, tokens, width, col_of, scaling,
    me_ref, order_any, q_ref, qt_ref, do_ref, peer_ref, *rest
):
    kv_refs = rest[:n_kv]
    dq_ref, sq_ref = rest[n_kv : n_kv + 2]
    out_refs = rest[n_kv + 2 : n_kv + 2 + n_out]
    rest = rest[n_kv + 2 + n_out :]
    groups = width // HD
    tiles = width // ROWS
    qs, kvs, kts, acc, sem, order_ref = rest[:6]
    rest = rest[6:]
    dqs, xs, rest = rest[:tiles], rest[tiles : 2 * tiles], rest[2 * tiles :]
    held = 5 * tiles + 1
    sets = len(rest) // held
    rest = [rest[w * held : (w + 1) * held] for w in range(sets)] * (3 - sets)
    stats_sets = [r[0] for r in rest]
    mcs = [r[1 : 1 + tiles] for r in rest]
    scores = [[r[1 + tiles + 4 * t :][:4] for t in range(tiles)] for r in rest]
    per_tile = ROWS // tokens
    me = me_ref[0]
    first = col_of(me)

    table = pltpu.make_async_copy(order_any, order_ref, sem.at[1])
    table.start()
    copies = []
    for which, ref in enumerate((q_ref, qt_ref, do_ref)):
        for g in range(groups):
            copies.append(
                pltpu.make_async_copy(
                    ref.at[:, pl.ds(pl.multiple_of(first + g * HD, HD), HD)],
                    qs.at[0, g // per_tile, which, pl.ds((g % per_tile) * tokens, tokens), :],
                    sem.at[0],
                )
            )
            copies.append(
                pltpu.make_async_copy(
                    peer_ref.at[:, pl.ds(which * width + g * HD, HD)],
                    qs.at[1, g // per_tile, which, pl.ds((g % per_tile) * tokens, tokens), :],
                    sem.at[0],
                )
            )
    for c in copies:
        c.start()
    acc[...] = jnp.zeros_like(acc)
    sq_ref[...] = jnp.zeros_like(sq_ref)
    table.wait()
    late = []
    for m, ref in enumerate(kv_refs):
        for e in range(ref.shape[0]):
            at = order_ref[seq_of(me, m, e)]
            late.append(pltpu.make_async_copy(ref.at[e], kvs.at[at], sem.at[0]))
    for c in late:
        c.start()
    copies += late
    for c in copies:
        c.wait()

    blocks = kvs.shape[0]
    per_chunk = CHUNK // tokens
    chunks = blocks // per_chunk

    def chunk_kv(kc):
        return kvs[pl.ds(kc * per_chunk, per_chunk)].reshape(CHUNK, 4 * HD)

    def transpose_keys(kc):
        kv = chunk_kv(kc)
        kts[kc, :, :CHUNK] = kv[:, :HD].T
        kts[kc, :, CHUNK:] = kv[:, HD : 2 * HD].T

    scale2 = scaling * LOG2E
    key_iota = lax.broadcasted_iota(jnp.int32, (CHUNK, ROWS), 0)
    row_iota = lax.rem(lax.broadcasted_iota(jnp.int32, (CHUNK, ROWS), 1), tokens)
    behind = row_iota - key_iota

    def split(x):
        return x.reshape(x.shape[0] // 8, 8, x.shape[1])

    piece = 32

    def score_dots(w, i, t, kc, masked, b, n):
        s_s, st_s, dp_s, dpt_s = scores[w][t]
        q, qt, do = qs[i, t, 0], qs[i, t, 1], qs[i, t, 2]
        kv = chunk_kv(kc)[:n]
        s = dot(kv[:, :HD], q, NT)
        if masked:
            s = jnp.where(behind[:n] >= kc * CHUNK - b * tokens, s, FILL)
        s_s[kc, :n] = s
        st_s[kc, :n] = dot(kv[:, : 2 * HD], jnp.concatenate([qt, q], axis=1), NT)
        both = dot(
            jnp.concatenate([kv[:, 2 * HD : 3 * HD], kv[:, 3 * HD :]], axis=0), do, NT
        )
        dp_s[kc, :n] = both[:n]
        dpt_s[kc, :n] = both[n:]

    def score_sums(w, t, kc, n):
        s_s, st_s, dp_s, dpt_s = scores[w][t]
        stats = stats_sets[w]
        m_old, z, s1, d1, x1, y1 = [stats[t, j] for j in range(6)]
        m_new = m_old
        for k in range(0, n, piece):
            s = split(s_s[kc, k : k + piece])
            m_new = jnp.maximum(m_new, jnp.max(s, axis=0) * scale2)
        decay = jnp.exp2(m_old - m_new)
        mcs[w][t][kc] = m_new
        z, s1, d1, x1, y1 = [v * decay for v in (z, s1, d1, x1, y1)]
        for k in range(0, n, piece):
            at = slice(k, k + piece)
            e = jnp.exp2(split(s_s[kc, at]) * scale2 - m_new[None])
            s_s[kc, at] = e.reshape(piece, ROWS)
            est = e * split(st_s[kc, at])
            dp = split(dp_s[kc, at])
            z = z + jnp.sum(e, axis=0)
            s1 = s1 + jnp.sum(est, axis=0)
            d1 = d1 + jnp.sum(e * dp, axis=0)
            x1 = x1 + jnp.sum(est * dp, axis=0)
            y1 = y1 + jnp.sum(e * split(dpt_s[kc, at]), axis=0)
        for j, v in enumerate((m_new, z, s1, d1, x1, y1)):
            stats[t, j] = v

    def finish(w, t):
        stats = stats_sets[w]
        m8, z, s1, d1, x1, y1 = [stats[t, j] for j in range(6)]
        top = jnp.max(m8, axis=0, keepdims=True)
        w8 = jnp.exp2(m8 - top)

        def total(v):
            return jnp.sum(v * w8, axis=0, keepdims=True)

        rz = 1.0 / total(z)
        tan_mean = total(s1) * rz
        delta = total(d1) * rz
        delta_tan = scaling * (total(x1) * rz - tan_mean * delta) + total(y1) * rz
        for j, v in enumerate((top, rz, tan_mean, delta, delta_tan)):
            stats[t, j] = jnp.broadcast_to(v, (8, ROWS))

    def grad_values(w, t, kc, n):
        s_s, st_s, dp_s, dpt_s = scores[w][t]
        stats = stats_sets[w]
        top, rz, tan_mean, delta, delta_tan = [stats[t, j] for j in range(5)]
        f = jnp.exp2(mcs[w][t][kc] - top) * rz
        fc = f * scaling
        for k in range(0, n, piece):
            at = slice(k, k + piece)
            e = split(s_s[kc, at])
            p = e * f[None]
            pt = e * fc[None] * (split(st_s[kc, at]) - tan_mean[None])
            dd = split(dp_s[kc, at]) - delta[None]
            dst = pt * dd + p * (split(dpt_s[kc, at]) - delta_tan[None])
            for j, v in enumerate((dst, p * dd, pt)):
                xs[t][j, at] = v.reshape(piece, ROWS).astype(jnp.bfloat16)

    def grad_dots(i, t, kc, n):
        q, qt, do = qs[i, t, 0], qs[i, t, 1], qs[i, t, 2]
        dst, ds, pt = xs[t][0, :n], xs[t][1, :n], xs[t][2, :n]
        keys_t = jnp.concatenate([kts[kc, :, :n], kts[kc, :, CHUNK : CHUNK + n]], axis=1)
        dqs[t][...] += dot(keys_t, jnp.concatenate([dst, ds], axis=0), NN)
        dk = dot(jnp.concatenate([dst, ds], axis=1), jnp.concatenate([q, qt], axis=0), NN)
        dv = dot(pt, do, NN)
        at = pl.ds(kc * per_chunk, n // tokens)
        acc[at, :, :HD] += dk.reshape(n // tokens, tokens, HD)
        acc[at, :, HD:] += dv.reshape(n // tokens, tokens, HD)

    def score_step(kc, _, w, i, b, masked, n=CHUNK):
        score_dots(w, i, 0, kc, masked, b, n)
        transpose_keys(kc)
        for t in range(tiles):
            if t + 1 < tiles:
                score_dots(w, i, t + 1, kc, masked, b, n)
            score_sums(w, t, kc, n)
        return 0

    def grad_step(kc, _, w, i, n=CHUNK):
        for t in range(tiles):
            grad_values(w, t, kc, n)
            grad_dots(i, t, kc, n)
        return 0

    def both_step(kc, _):
        for t in range(tiles):
            score_dots(1, i1, t, kc, False, b1, CHUNK)
            grad_values(0, t, kc, CHUNK)
            grad_dots(i0, t, kc, CHUNK)
            score_sums(1, t, kc, CHUNK)
        return 0

    def tail(kc, b, step, **fixed):
        short = lax.rem(b, per_chunk) * tokens < CHUNK // 2

        @pl.when(short)
        def _():
            step(kc, 0, n=CHUNK // 2, **fixed)

        @pl.when(jnp.logical_not(short))
        def _():
            step(kc, 0, n=CHUNK, **fixed)

    def clear(w):
        stats_sets[w][...] = jnp.zeros_like(stats_sets[w])
        for t in range(tiles):
            stats_sets[w][t, 0] = jnp.full((8, ROWS), FILL, jnp.float32)

    def clear_dq():
        for t in range(tiles):
            dqs[t][...] = jnp.zeros_like(dqs[t])

    def store_dq(i):
        for t in range(tiles):
            dq = (dqs[t][...] * scaling).T.astype(jnp.bfloat16)
            wide = dq.astype(jnp.float32)
            sq_ref[...] += jnp.sum(split(wide * wide), axis=0)
            for h in range(per_tile):
                c = (t * per_tile + h) * HD
                dq_ref[i, :, c : c + HD] = dq[h * tokens : (h + 1) * tokens]

    def run(low, high, step, **fixed):
        lax.fori_loop(low, high, functools.partial(step, **fixed), 0)

    own, peer = order_ref[me], order_ref[me ^ 1]
    i0 = (own > peer).astype(jnp.int32)
    i1 = 1 - i0
    b0, b1 = jnp.minimum(own, peer), jnp.maximum(own, peer)
    full0, full1 = (b0 * tokens) // CHUNK, (b1 * tokens) // CHUNK
    clear(0)
    run(0, full0, score_step, w=0, i=i0, b=b0, masked=False)
    tail(full0, b0, functools.partial(score_step, w=0, i=i0, b=b0, masked=True))
    for t in range(tiles):
        finish(0, t)
    clear_dq()
    joint = 0
    if sets > 1:
        clear(1)
        joint = jnp.minimum(full0, full1)
        run(0, joint, both_step)
    run(joint, full0, grad_step, w=0, i=i0)
    tail(full0, b0, functools.partial(grad_step, w=0, i=i0))
    store_dq(i0)
    clear_dq()
    if sets == 1:
        clear(1)
    run(joint, full1, score_step, w=1, i=i1, b=b1, masked=False)
    tail(full1, b1, functools.partial(score_step, w=1, i=i1, b=b1, masked=True))
    for t in range(tiles):
        finish(1, t)
    run(0, full1, grad_step, w=1, i=i1)
    tail(full1, b1, functools.partial(grad_step, w=1, i=i1))
    store_dq(i1)

    for m, ref in enumerate(out_refs):
        for e in range(ref.shape[0] // tokens):
            block_at = acc[order_ref[out_seq(me, m, e)]]
            rows_at = slice(e * tokens, (e + 1) * tokens)
            ref[rows_at, :HD] = (block_at[:, :HD] * scaling).astype(ref.dtype)
            ref[rows_at, HD:] = block_at[:, HD:].astype(ref.dtype)


def run_hvp(me, order, q, qt, do, peer, kvs, outs, seq_of, out_seq, col_of, width):
    tokens = q.shape[0]
    blocks = sum(k.shape[0] for k in kvs)
    chunks = blocks * tokens // CHUNK
    tiles = width // ROWS
    f32 = jnp.float32
    score = pltpu.VMEM((chunks, CHUNK, ROWS), f32)
    sets = 2 if 2 * 4 * tiles * chunks * CHUNK * ROWS * 4 <= 36 << 20 else 1
    kernel = functools.partial(
        hvp_kernel, seq_of, out_seq, len(kvs), len(outs), tokens, width, col_of, HD ** (-0.5)
    )
    outs = [
        jax.ShapeDtypeStruct((2, tokens, width), jnp.bfloat16),
        jax.ShapeDtypeStruct((8, HD), f32),
    ] + outs
    flops = 2 * blocks * tokens * tokens * width * 10
    return pl.pallas_call(
        kernel,
        name="hvp",
        out_shape=outs,
        in_specs=[pl.BlockSpec(memory_space=pltpu.SMEM)]
        + [pl.BlockSpec(memory_space=pl.ANY)] * (5 + len(kvs)),
        out_specs=[pl.BlockSpec(memory_space=pltpu.VMEM)] * len(outs),
        scratch_shapes=[
            pltpu.VMEM((2, tiles, 3, ROWS, HD), jnp.bfloat16),
            pltpu.VMEM((blocks, tokens, 4 * HD), jnp.bfloat16),
            pltpu.VMEM((chunks, HD, 2 * CHUNK), jnp.bfloat16),
            pltpu.VMEM((blocks, tokens, 2 * HD), f32),
            pltpu.SemaphoreType.DMA((2,)),
            pltpu.SMEM(order.shape, jnp.int32),
        ]
        + [pltpu.VMEM((HD, ROWS), f32)] * tiles
        + [pltpu.VMEM((3, CHUNK, ROWS), jnp.bfloat16)] * tiles
        + sets
        * (
            [pltpu.VMEM((tiles, 6, 8, ROWS), f32)]
            + [pltpu.VMEM((chunks, 8, ROWS), f32)] * tiles
            + [score] * (4 * tiles)
        ),
        compiler_params=pltpu.CompilerParams(vmem_limit_bytes=48 * 1024 * 1024),
        cost_estimate=pl.CostEstimate(flops=flops, bytes_accessed=4 << 20, transcendentals=0),
    )(me, order, q, qt, do, peer, *kvs)


def add_kernel(me_ref, own_ref, *rest):
    *got, dq_ref, dq_got_ref, sq_ref, dq_out, mine_ref, peer_ref, sum_ref, sem = rest
    width = dq_ref.shape[2]
    tokens = dq_ref.shape[1]
    core = lax.rem(me_ref[0], 2)
    mine = pl.multiple_of(core * width, HD)
    theirs = pl.multiple_of((1 - core) * width, HD)
    moves = (
        pltpu.make_async_copy(dq_ref.at[0], dq_out.at[:, pl.ds(mine, width)], sem.at[0]),
        pltpu.make_async_copy(dq_got_ref, dq_out.at[:, pl.ds(theirs, width)], sem.at[1]),
    )
    for move in moves:
        move.start()
    f32 = jnp.float32
    total = sq_ref[...]
    for e, out in enumerate((mine_ref, peer_ref)):
        rows = slice(e * tokens, (e + 1) * tokens)
        for cols in (slice(0, HD), slice(HD, 2 * HD)):
            final = own_ref[rows, cols]
            for ref in got:
                final = final + ref[rows, cols].astype(f32)
            final = final.astype(jnp.bfloat16)
            out[:, cols] = final
            wide = final.astype(f32)
            total = total + jnp.sum((wide * wide).reshape(-1, 8, HD), axis=0)
    line = jnp.sum(total, axis=0, keepdims=True)
    sum_ref[...] = jnp.broadcast_to(line[None], sum_ref.shape)
    for move in moves:
        move.wait()


def run_add(me, own, got, dq, dq_got, sq, devices):
    tokens, width = dq.shape[1:]
    half = jax.ShapeDtypeStruct((tokens, 2 * HD), jnp.bfloat16)
    return pl.pallas_call(
        add_kernel,
        name="add",
        out_shape=[
            jax.ShapeDtypeStruct((tokens, 2 * width), jnp.bfloat16),
            half,
            half,
            jax.ShapeDtypeStruct((devices, 1, HD), jnp.float32),
        ],
        in_specs=[pl.BlockSpec(memory_space=pltpu.SMEM)]
        + [pl.BlockSpec(memory_space=pltpu.VMEM)] * (len(got) + 4),
        out_specs=[pl.BlockSpec(memory_space=pl.ANY)]
        + [pl.BlockSpec(memory_space=pltpu.VMEM)] * 3,
        scratch_shapes=[pltpu.SemaphoreType.DMA((2,))],
        compiler_params=pltpu.CompilerParams(vmem_limit_bytes=4 << 20),
        cost_estimate=pl.CostEstimate(flops=1 << 20, bytes_accessed=2 << 20, transcendentals=0),
    )(me, own, *got, dq, dq_got, sq)


def in_hbm(x):
    return pltpu.with_memory_space_constraint(x, pltpu.HBM)


def pack_kernel(count, me_ref, order_ref, *refs):
    core = lax.rem(me_ref[0], 2)
    sources, rows = refs[:count], refs[count:-5]
    theirs_ref, mine_ref, rows_ref, table_ref, sem = refs[-5:]
    moves = [pltpu.make_async_copy(order_ref, table_ref, sem.at[0])]

    def move(ref, at, width, out, to):
        cols = pl.ds(pl.multiple_of(at * width, HD), width)
        moves.append(
            pltpu.make_async_copy(
                ref.at[:, cols], out.at[:, pl.ds(to * width, width)], sem.at[len(moves)]
            )
        )

    for out, head in ((theirs_ref, 1 - core), (mine_ref, core)):
        for j, ref in enumerate(sources):
            move(ref, head, HD, out, j)
    for j, ref in enumerate(rows):
        move(ref, 1 - core, ref.shape[1] // 2, rows_ref, j)
    for m in moves:
        m.start()
    for m in moves:
        m.wait()


def run_pack(me, order, sources, rows):
    tokens = rows[0].shape[0]
    half = pltpu.VMEM((tokens, len(sources) * HD), sources[0].dtype)
    wide = pltpu.VMEM((tokens, sum(r.shape[1] for r in rows) // 2), rows[0].dtype)
    count = 1 + 2 * len(sources) + len(rows)
    return pl.pallas_call(
        functools.partial(pack_kernel, len(sources)),
        name="pack",
        out_shape=[half, half, wide, pltpu.VMEM(order.shape, order.dtype)],
        in_specs=[pl.BlockSpec(memory_space=pltpu.SMEM)]
        + [pl.BlockSpec(memory_space=pltpu.HBM)] * (1 + len(sources) + len(rows)),
        out_specs=[pl.BlockSpec(memory_space=pltpu.VMEM)] * 4,
        scratch_shapes=[pltpu.SemaphoreType.DMA((count,))],
        compiler_params=pltpu.CompilerParams(vmem_limit_bytes=4 << 20),
        cost_estimate=pl.CostEstimate(flops=1 << 16, bytes_accessed=1 << 21, transcendentals=0),
    )(me, *map(in_hbm, (order, *sources, *rows)))


def last_kernel(me_ref, mine_ref, got_ref, lines_ref, dk_out, dv_out, norm_ref):
    core = lax.rem(me_ref[0], 2)
    for ref, at in ((mine_ref, core), (got_ref, 1 - core)):
        cols = pl.ds(pl.multiple_of(at * HD, HD), HD)
        dk_out[:, cols] = ref[:, :HD]
        dv_out[:, cols] = ref[:, HD:]
    norm_ref[0, 0] = jnp.sum(lines_ref[...])


def run_last(me, mine, got, lines):
    return pl.pallas_call(
        last_kernel,
        name="last",
        out_shape=[
            jax.ShapeDtypeStruct(mine.shape, mine.dtype),
            jax.ShapeDtypeStruct(mine.shape, mine.dtype),
            jax.ShapeDtypeStruct((1, 1), jnp.float32),
        ],
        in_specs=[pl.BlockSpec(memory_space=pltpu.SMEM)]
        + [pl.BlockSpec(memory_space=pltpu.VMEM)] * 3,
        out_specs=[pl.BlockSpec(memory_space=pltpu.VMEM)] * 2
        + [pl.BlockSpec(memory_space=pltpu.SMEM)],
        compiler_params=pltpu.CompilerParams(vmem_limit_bytes=4 << 20),
        cost_estimate=pl.CostEstimate(flops=1 << 16, bytes_accessed=1 << 18, transcendentals=0),
    )(me, mine, got, lines)


def shifted(x, axis, bit):
    size = lax.axis_size(axis)
    return lax.ppermute(x, axis, [(i, i ^ bit) for i in range(size)])


def all_sum(x, axes):
    for axis in axes:
        size = lax.axis_size(axis)
        if size & (size - 1):
            x = lax.psum(x, axis)
            continue
        bit = 1
        while bit < size:
            x = x + shifted(x, axis, bit)
            bit *= 2
    return x


def square_sum(x):
    w = x.astype(jnp.float32)
    return jnp.sum(w * w)


def join(core, mine, theirs):
    low = jnp.where(core == 0, mine, theirs)
    high = jnp.where(core == 0, theirs, mine)
    return jnp.concatenate([low, high], axis=1)


def body(queries, keys, values, q_tangent, k_tangent, v_tangent, out_grad, block_order):
    tokens = queries.shape[0]
    heads = keys.shape[1] // HD
    shards = lax.axis_size("seq")
    me = lax.axis_index("seq").astype(jnp.int32)
    core = lax.rem(me, 2)
    me_arr = me.reshape(1)
    width = heads * G * HD // 2
    other = (1 - core) * width
    f32 = jnp.float32

    def swap_rows(arrays):
        cut = [lax.dynamic_slice_in_dim(x, other, width, 1) for x in arrays]
        return shifted(jnp.concatenate(cut, axis=1), "seq", 1)

    rows = (queries, q_tangent, out_grad)

    def col_of(at):
        return lax.rem(at, 2) * width

    sources = (keys, k_tangent, values, v_tangent)


    if heads == 2 and shards == 8:
        theirs, mine, cut, table = run_pack(me_arr, block_order, sources, rows)
        peer_kv = shifted(theirs, "seq", 1)
        x_kv = [shifted(mine, "seq", 2), shifted(theirs, "seq", 3)]
        y_kv = [shifted(mine, "seq", 4), shifted(theirs, "seq", 5)]
        peer_rows = shifted(cut, "seq", 1)
        half = 2 * HD
        xy_a = shifted(jnp.stack([v[:, :half] for v in y_kv]), "seq", 2)
        xy_b = shifted(jnp.stack([v[:, half:] for v in x_kv]), "seq", 4)
        xy_kv = jnp.concatenate([xy_a, xy_b], axis=2)
        kvs = [v[None] for v in (mine, peer_kv, *x_kv, *y_kv)] + [xy_kv]
        dq, sq, own, *parts = run_hvp(
            me_arr, table, *rows, peer_rows, kvs,
            [jax.ShapeDtypeStruct((2 * tokens, 2 * HD), f32)]
            + [jax.ShapeDtypeStruct((2 * tokens, 2 * HD), jnp.bfloat16)] * (shards // 2 - 1),
            lambda at, m, e: at ^ (m + e), lambda at, m, e: at ^ (2 * m + e), col_of, width,
        )
        got = [shifted(p, "seq", 2 * m + 2) for m, p in enumerate(parts)]
        dq_got = shifted(dq[1], "seq", 1)
        devices = shards * lax.axis_size("head")
        dq_out, dkv_mine, dkv_peer, line = run_add(me_arr, own, got, dq, dq_got, sq, devices)
        dkv_got = shifted(dkv_peer, "seq", 1)
        lines = lax.all_to_all(line, ("head", "seq"), 0, 0)
        dk_out, dv_out, norm = run_last(me_arr, dkv_mine, dkv_got, lines)
        return (dq_out, dk_out, dv_out, norm[0, 0])
    assert heads == 1
    whole = lax.all_gather(jnp.concatenate(sources, axis=1), "seq", axis=0)
    dq, sq, parts = run_hvp(
        me_arr, block_order, *rows, swap_rows(rows), (whole,),
        [jax.ShapeDtypeStruct((shards * tokens, 2 * HD), jnp.bfloat16)],
        lambda at, m, e: e, lambda at, m, e: e, col_of, width,
    )
    final = lax.psum_scatter(parts, "seq", scatter_dimension=0, tiled=True)
    dq_out = join(core, dq[0], shifted(dq[1], "seq", 1))
    local = square_sum(final) + jnp.sum(sq)
    squared_norm = all_sum(local, ("seq", "head"))
    return (dq_out, final[:, :HD], final[:, HD:], squared_norm)


def solution(mesh):
    placed = (P("seq", "head"),) * 7 + (P(),)
    return jax.shard_map(
        body,
        mesh=mesh,
        in_specs=placed,
        out_specs=(P("seq", "head"), P("seq", "head"), P("seq", "head"), P()),
        check_vma=False,
    )
```
